32 devices in a mesh: leaf: 32 (over z, y, x, core).
Axes of the slice: x: 2, y: 2, z: 4, core: 2. Of those that a mesh axis runs over, the one named last changes fastest.
Arguments:
- slip: bfloat16 [128, 8192], P(None, 'leaf'), may hold values from -6 to 6
- to_multipole: bfloat16 [121, 128], replicated, may hold values from -0.5 to 0.5
- up_shift: float32 [2, 121, 121], replicated, may hold values from -0.375 to 0.375
- down_shift: float32 [2, 121, 121], replicated, may hold values from -0.5 to 0.5
- sibling_far: float32 [2, 121, 121], replicated, may hold values from -0.5 to 0.5
- leaf_far: bfloat16 [27, 121, 121], replicated, may hold values from -0.25 to 0.25
- to_stress: bfloat16 [128, 121], replicated, may hold values from -0.125 to 0.125
- near_blocks: bfloat16 [9, 128, 128], replicated, may hold values from -0.1875 to 0.1875
- send_cells: int32 [32, 4096], P('leaf'), may hold values from 0 to 255, as said below
- far_list: int32 [27, 8192], P(None, 'leaf'), may hold values from 0 to 4351, as said below
- near_list: int32 [9, 8192], P(None, 'leaf'), may hold values from 0 to 319, as said below
Outputs:
- stress: float32 [128, 8192], P(None, 'leaf')
The draws below stay inside these ranges and needn't reach their ends.
Inputs may be any that keep to these rules, and one draw needn't show every extreme that they name: `send_cells`: row q holds, in positions d * 128 to (d + 1) * 128 - 1, 128 distinct cells of device q (numbered within that device) listed for receiving device d. `far_list`: an entry v below 256 names a cell of the target's own device. Otherwise v - 256 = q * 128 + s names slot s of device q's list for the target's device, q is not the target's device, s < 128 when q lies within 4 devices of it and s < 32 when it lies farther; in every draw some entry names slot 127 of a device within 4, and some names slot 31 of a farther device. `near_list`: an entry w names the cell w - 32 counted from the first cell of the target's device, so that positions before 0 and from 256 on lie on the neighbouring devices (zeros outside the fault); entry 4 is the target itself.
All inputs are finite; a program needn't handle non-finite values.
Results may differ from the reference program's by a relative error of at most 0.0031.
Values may be sent and summed in bfloat16 or wider, within the bound.
A program may use at most 64 MiB of HBM per device.

```python
import jax
import jax.numpy as jnp
from jax import lax

ELEM = 128
COEF = 121
NEAR = 9
TYPES = 27
NEAR_PEERS = 4
CELLS_DEV = 256
HALO = 32
CAP_NEAR = 128
CAP_FAR = 32
CELLS = 8192
N_LEAF = 32


def let_plan(key):
    base = jax.random.fold_in(key, 4127)
    keys = jax.random.split(base, 5)
    devices_all = N_LEAF
    receiver = jnp.arange(devices_all, dtype=jnp.int32)[:, None]
    sender = jnp.arange(devices_all, dtype=jnp.int32)[None, :]
    apart = jnp.abs(sender - receiver)
    close_count = jax.random.randint(keys[0], (devices_all, devices_all), CAP_NEAR // 4, CAP_NEAR + 1)
    far_count = jax.random.randint(keys[1], (devices_all, devices_all), CAP_FAR // 2, CAP_FAR + 1)
    counts = jnp.where(apart == 0, 0, jnp.where(apart <= NEAR_PEERS, close_count, far_count))
    counts = jnp.where(sender == receiver + 1, CAP_NEAR, counts)
    counts = jnp.where(sender == (receiver + devices_all // 2) % devices_all, CAP_FAR, counts)
    scores = jax.random.randint(keys[2], (devices_all, devices_all, CELLS_DEV), 0, 1 << 20)
    scores = scores * CELLS_DEV + jnp.arange(CELLS_DEV, dtype=jnp.int32)
    chosen = jnp.argsort(scores, axis=-1)[:, :, :CAP_NEAR].astype(jnp.int32)
    send_lists = chosen.reshape(devices_all, devices_all * CAP_NEAR)
    entries = TYPES * CELLS_DEV
    position = jnp.arange(CAP_NEAR, dtype=jnp.int32)
    usable = (position[None, None, :] < counts[:, :, None]).reshape(devices_all, devices_all * CAP_NEAR)
    codes = CELLS_DEV + jnp.arange(devices_all * CAP_NEAR, dtype=jnp.int32)
    ranks = jnp.cumsum(usable.astype(jnp.int32), axis=1) - 1
    place_scores = jax.random.randint(keys[3], (devices_all, entries - 1), 0, 1 << 14)
    place_scores = place_scores * entries + jnp.arange(entries - 1, dtype=jnp.int32)
    places = 1 + jnp.argsort(place_scores, axis=1).astype(jnp.int32)
    targets = jnp.take_along_axis(places, jnp.clip(ranks, 0, entries - 2), axis=1)
    targets = jnp.where(usable, targets, entries)
    own_cells = jax.random.randint(keys[4], (devices_all, entries), 0, CELLS_DEV)
    own_cells = own_cells.at[:, 0].set(0)
    rows = jnp.broadcast_to(receiver, targets.shape)
    filled = own_cells.at[rows, targets].set(jnp.broadcast_to(codes[None, :], targets.shape), mode='drop')
    lists = filled.reshape(devices_all, TYPES, CELLS_DEV).transpose(1, 0, 2).reshape(TYPES, devices_all * CELLS_DEV)
    return (send_lists.astype(jnp.int32), lists.astype(jnp.int32))


def draw_send_cells(key, part):
    return let_plan(key)[0]


def draw_far_list(key, part):
    return let_plan(key)[1]


def draw_near_list(key, part):
    base = jax.random.fold_in(key, 9151)
    cells_here = jnp.arange(CELLS_DEV, dtype=jnp.int32)
    jumps = jax.random.randint(base, (NEAR, N_LEAF, CELLS_DEV), -HALO, HALO + 1)
    kinds = jnp.arange(NEAR, dtype=jnp.int32)[:, None, None]
    jumps = jnp.where(kinds == NEAR // 2, 0, jumps)
    values = cells_here[None, None, :] + HALO + jumps
    values = values.at[0, :, 0].set(0)
    values = values.at[NEAR - 1, :, CELLS_DEV - 1].set(CELLS_DEV + 2 * HALO - 1)
    return values.reshape(NEAR, N_LEAF * CELLS_DEV).astype(jnp.int32)


def level_of(stream_key, extent, cuts, least, largest):
    def one(dim, shards_of):
        steps = jax.random.uniform(jax.random.fold_in(jax.random.fold_in(stream_key, 6), dim), (shards_of,), jnp.float32, least / len(cuts), largest / len(cuts))
        return jnp.repeat(jnp.exp(steps), extent[dim] // shards_of).reshape((-1,) + (1,) * (len(extent) - dim - 1))

    loudness = one(*cuts[0])
    for cut in cuts[1:]:
        loudness = loudness * one(*cut)
    return loudness


def noise(stream_key, dims, spread, bound, pieces=(), kind=jnp.bfloat16):
    values = spread * jax.random.normal(stream_key, dims, jnp.float32)
    if pieces:
        values = values * level_of(stream_key, dims, pieces, -0.22, 0.18)
    return jnp.clip(values, -bound, bound).astype(kind)


def setup_inputs(seed: int = 0) -> dict:
    key_of = jax.random.split(jax.random.key(seed), 12)
    return {
        "slip": noise(key_of[0], (ELEM, CELLS), 1.0, 6.0, ((1, 32),)),
        "to_multipole": noise(key_of[1], (COEF, ELEM), ELEM ** -0.5, 0.5),
        "up_shift": noise(key_of[2], (2, COEF, COEF), (2 * COEF) ** -0.5, 0.375, (), jnp.float32),
        "down_shift": noise(key_of[3], (2, COEF, COEF), COEF ** -0.5, 0.5, (), jnp.float32),
        "sibling_far": noise(key_of[4], (2, COEF, COEF), COEF ** -0.5, 0.5, (), jnp.float32),
        "leaf_far": noise(key_of[5], (TYPES, COEF, COEF), (4 * COEF) ** -0.5, 0.25),
        "to_stress": noise(key_of[6], (ELEM, COEF), (16 * COEF) ** -0.5, 0.125),
        "near_blocks": noise(key_of[7], (NEAR, ELEM, ELEM), (NEAR * ELEM) ** -0.5, 0.1875),
        "send_cells": draw_send_cells(jax.random.fold_in(key_of[11], 71), 0),
        "far_list": draw_far_list(jax.random.fold_in(key_of[11], 71), 0),
        "near_list": draw_near_list(jax.random.fold_in(key_of[11], 71), 0),
    }


def reference(slip, to_multipole, up_shift, down_shift, sibling_far, leaf_far, to_stress, near_blocks, send_cells, far_list, near_list):
    precise = lax.Precision.HIGHEST
    multipole = jnp.dot(to_multipole, slip, preferred_element_type=jnp.float32).astype(jnp.bfloat16)
    heights = CELLS.bit_length() - 1
    aggregates = [multipole.astype(jnp.float32)]
    for height in range(heights - 1):
        below = aggregates[-1]
        aggregates.append(jnp.dot(up_shift[0], below[:, 0::2], precision=precise)
                          + jnp.dot(up_shift[1], below[:, 1::2], precision=precise))
    expansion = jnp.zeros((COEF, 1), jnp.float32)
    for height in range(heights - 1, -1, -1):
        left_part = jnp.dot(down_shift[0], expansion, precision=precise)
        right_part = jnp.dot(down_shift[1], expansion, precision=precise)
        if height >= 1:
            level_sums = aggregates[height]
            left_part = left_part + jnp.dot(sibling_far[0], level_sums[:, 1::2], precision=precise)
            right_part = right_part + jnp.dot(sibling_far[1], level_sums[:, 0::2], precision=precise)
        expansion = jnp.stack([left_part, right_part], axis=-1).reshape(COEF, -1)
    owner = jnp.arange(CELLS, dtype=jnp.int32) // CELLS_DEV
    relative = far_list - CELLS_DEV
    sender = jnp.clip(relative // CAP_NEAR, 0, N_LEAF - 1).astype(jnp.int32)
    position = (relative % CAP_NEAR).astype(jnp.int32)
    flat_lists = send_cells.reshape(-1)
    listed = flat_lists[sender * (N_LEAF * CAP_NEAR) + owner[None, :] * CAP_NEAR + position]
    source = jnp.where(far_list < CELLS_DEV, owner[None, :] * CELLS_DEV + far_list, sender * CELLS_DEV + listed).astype(jnp.int32)
    leaf_sum = jnp.zeros((COEF, CELLS), jnp.float32)
    for kind in range(TYPES):
        leaf_sum = leaf_sum + jnp.dot(leaf_far[kind], jnp.take(multipole, source[kind], axis=1), preferred_element_type=jnp.float32)
    local_exp = (expansion + leaf_sum).astype(jnp.bfloat16)
    padded = jnp.pad(slip, ((0, 0), (HALO, HALO)))
    near_source = (owner[None, :] * CELLS_DEV + near_list).astype(jnp.int32)
    stress = jnp.dot(to_stress, local_exp, preferred_element_type=jnp.float32)
    for kind in range(NEAR):
        stress = stress + jnp.dot(near_blocks[kind], jnp.take(padded, near_source[kind], axis=1), preferred_element_type=jnp.float32)
    return stress
```

```python
import functools

import jax
import jax.numpy as jnp
from jax import lax
from jax.experimental import pallas as pl
from jax.experimental.pallas import tpu as pltpu
from jax.sharding import PartitionSpec as P

HALO = 32
PEERS = 4
CAP_FAR = 32
LANES = 128
BF = jnp.bfloat16
F32 = jnp.float32
MESH = pl.DeviceIdType.MESH
OFFSETS = tuple(range(-PEERS, 0)) + tuple(range(1, PEERS + 1))


def mm(a, b):
    return jnp.dot(a, b, preferred_element_type=F32)


def halves(x):
    high = x.astype(BF)
    return high, (x - high.astype(F32)).astype(BF)


def one_hot(rows, index):
    count = index.shape[1]
    lines = lax.broadcasted_iota(jnp.int32, (rows, count), 0).astype(F32).astype(BF)
    hit = lines == jnp.broadcast_to(index.astype(BF), (rows, count))
    return jnp.where(hit, jnp.ones((), BF), jnp.zeros((), BF))


def kernel(
    n, cells, cap,
    slip_any, tm_any, up_any, down_any, sib_any, leaf_any, ts_any, nb_any, send_any, far_any, near_any,
    out_ref,
    slip_ref, tm_ref, up_ref, down_ref, sib_ref, leaf_ref, ts_ref, nb_ref, send_ref, far_ref, near_ref,
    far_out, near_out, far_buf, near_buf, edges, halo, root_out, roots, send_f, far_idx,
    weight, w_up, w_sib, w_down, agg, terms, loc, rel, near_rel, source, leaf_cat, columns, near_cols, load_sem,
    far_send, far_recv, near_send, near_recv, halo_send, halo_recv, root_send, root_recv,
):
    me = lax.axis_index("leaf")
    coef = tm_ref.shape[0]
    types = far_ref.shape[0]
    kinds = near_ref.shape[0]
    rest = cap - CAP_FAR
    team = 256 // CAP_FAR
    teams = n // team
    mine = me // team

    pairs = (
        (slip_any, slip_ref), (tm_any, tm_ref), (send_any, send_ref), (up_any, up_ref), (sib_any, sib_ref),
        (far_any, far_ref), (near_any, near_ref), (down_any, down_ref), (leaf_any, leaf_ref), (nb_any, nb_ref),
        (ts_any, ts_ref),
    )
    loads = [pltpu.make_async_copy(a, b, load_sem.at[i]) for i, (a, b) in enumerate(pairs)]
    for copy in loads:
        copy.start()

    barrier = pltpu.get_barrier_semaphore()

    far_buf[...] = jnp.zeros_like(far_buf)
    near_buf[...] = jnp.zeros_like(near_buf)
    halo[...] = jnp.zeros_like(halo)

    def greet(k, carry):
        pl.semaphore_signal(barrier, inc=1, device_id=(lax.rem(me + k, n),), device_id_type=MESH)
        return carry

    lax.fori_loop(1, n, greet, 0)

    weight[...] = jnp.zeros_like(weight)
    w_sib[...] = jnp.zeros_like(w_sib)
    for copy in loads[:3]:
        copy.wait()

    weight[0, :coef, :] = tm_ref[...].astype(F32)
    multipole = mm(weight[0].astype(BF), slip_ref[...]).astype(BF)
    source[:, :cells] = multipole
    edges[0] = slip_ref[:, :LANES].astype(F32).T[:HALO].astype(BF)
    edges[1] = slip_ref[:, cells - LANES :].astype(F32).T[LANES - HALO :].astype(BF)

    def far_copy(target):
        return pltpu.make_async_remote_copy(
            src_ref=far_out.at[pl.ds(pl.multiple_of(target * CAP_FAR, CAP_FAR), CAP_FAR)],
            dst_ref=far_buf.at[pl.ds(pl.multiple_of(me * CAP_FAR, CAP_FAR), CAP_FAR)],
            send_sem=far_send,
            recv_sem=far_recv.at[mine],
            device_id=(target,),
            device_id_type=MESH,
        )

    def far_rows(start, rows, team_index):
        return pltpu.make_async_remote_copy(
            src_ref=far_out.at[pl.ds(start, rows)],
            dst_ref=far_buf.at[pl.ds(start, rows)],
            send_sem=far_send,
            recv_sem=far_recv.at[team_index],
            device_id=(lax.rem(me + 1, n),),
            device_id_type=MESH,
        )

    def near_copy(j):
        target = jnp.clip(me + OFFSETS[j], 0, n - 1)
        back = len(OFFSETS) - 1 - j
        return pltpu.make_async_remote_copy(
            src_ref=near_out.at[pl.ds(j * cap + CAP_FAR, rest)],
            dst_ref=near_buf.at[pl.ds(back * rest, rest)],
            send_sem=near_send.at[j],
            recv_sem=near_recv.at[back],
            device_id=(target,),
            device_id_type=MESH,
        )

    def halo_copy(side):
        target = jnp.clip(me + (1 if side else -1), 0, n - 1)
        return pltpu.make_async_remote_copy(
            src_ref=edges.at[side],
            dst_ref=halo.at[pl.ds((1 - side) * HALO, HALO)],
            send_sem=halo_send.at[side],
            recv_sem=halo_recv.at[1 - side],
            device_id=(target,),
            device_id_type=MESH,
        )

    def root_copy(k):
        return pltpu.make_async_remote_copy(
            src_ref=root_out,
            dst_ref=roots.at[me],
            send_sem=root_send.at[k],
            recv_sem=root_recv.at[k],
            device_id=(lax.rem(me + k, n),),
            device_id_type=MESH,
        )

    def inside(offset):
        return jnp.logical_and(me + offset >= 0, me + offset < n)

    send_f[...] = send_ref[...].astype(F32)
    per_row = LANES // CAP_FAR
    strip = 8 * per_row
    lane = lax.broadcasted_iota(jnp.int32, (8, LANES), 1)
    for g in range(n // strip):
        packed = send_f[pl.ds(g * strip, 8, stride=per_row), :]
        for j in range(1, per_row):
            shifted = pltpu.roll(send_f[pl.ds(g * strip + j, 8, stride=per_row), :], j * CAP_FAR, axis=1)
            packed = jnp.where(lane >= j * CAP_FAR, shifted, packed)
        far_idx[g * 8 : (g + 1) * 8, :] = packed

    def pick(first, second):
        hits = jnp.concatenate([one_hot(cells, first), one_hot(cells, second)], axis=1)
        return mm(multipole, hits).T.astype(BF)

    for g in range(n // (2 * per_row)):
        far_out[g * 256 : (g + 1) * 256, :] = pick(far_idx[2 * g : 2 * g + 1, :], far_idx[2 * g + 1 : 2 * g + 2, :])

    for j in range(0, len(OFFSETS), 2):
        first, second = (
            send_f[pl.ds(jnp.clip(me + OFFSETS[i], 0, n - 1), 1), :] for i in (j, j + 1)
        )
        near_out[j * cap : (j + 2) * cap, :] = pick(first, second)

    pl.semaphore_wait(barrier, n - 1)

    for j, offset in enumerate(OFFSETS):
        @pl.when(inside(offset))
        def _():
            near_copy(j).start()

    def start_far(i, carry):
        target = (i // team) * team + lax.rem(me + i, team)

        @pl.when(target != me)
        def _():
            far_copy(target).start()

        return carry

    lax.fori_loop(0, n, start_far, 0)

    for side in (0, 1):
        @pl.when(inside(1 if side else -1))
        def _():
            halo_copy(side).start()

    for copy in loads[3:5]:
        copy.wait()

    def parts(ref, index):
        weight[index, :coef, :coef] = ref
        weight[index, :coef, coef:] = jnp.zeros((coef, LANES - coef), F32)
        return halves(weight[index].T)

    for s in (0, 1):
        high, low = parts(up_ref[:, s, :], 0 + s)
        w_up[s * LANES : (s + 1) * LANES, :LANES] = high
        w_up[s * LANES : (s + 1) * LANES, LANES:] = low
        high, low = parts(sib_ref[:, s, :], 4 + s)
        other = 1 - s
        w_sib[0, other * LANES : (other + 1) * LANES, s * LANES : (s + 1) * LANES] = high
        w_sib[1, other * LANES : (other + 1) * LANES, s * LANES : (s + 1) * LANES] = low

    def pair(base, rows):
        m = max(rows // 2, 8)
        even = agg[pl.ds(base, m, stride=2), :]
        odd = agg[pl.ds(base + 1, m, stride=2), :]
        return m, halves(jnp.concatenate([even, odd], axis=1))

    def lift(high, low):
        first = mm(high, w_up[...])
        second = mm(low, w_up[:, :LANES])
        return first[:, :LANES] + first[:, LANES:] + second

    def across(high, low):
        return mm(high, w_sib[0]) + mm(high, w_sib[1]) + mm(low, w_sib[0])

    def place(base, value):
        agg[base : base + value.shape[0], :] = value
        if value.shape[0] < 16:
            agg[base + value.shape[0] : base + 16, :] = jnp.zeros((16 - value.shape[0], LANES), F32)

    local_levels = cells.bit_length() - 1
    tree_bits = n.bit_length() - 1
    base, spot = 0, 0
    agg[:cells, :] = multipole.astype(F32).T
    local_spots = []
    for height in range(local_levels):
        rows = cells >> height
        m, (high, low) = pair(base, rows)
        if height >= 1:
            terms[spot : spot + m, :] = across(high, low)
            local_spots.append(spot)
            spot += m
        else:
            local_spots.append(None)
        value = lift(high, low)
        base += max(rows, 16)
        place(base, value)
    root_out[...] = value[:1]
    roots[me] = value[:1]

    def start_root(k, carry):
        root_copy(k).start()
        return carry

    lax.fori_loop(1, n, start_root, 0)

    for copy in loads[5:]:
        copy.wait()

    for s in (0, 1):
        high, low = parts(down_ref[:, s, :], 2 + s)
        w_down[:LANES, s * LANES : (s + 1) * LANES] = high
        w_down[LANES:, s * LANES : (s + 1) * LANES] = low

    v = far_ref[...]
    behind = v - cells
    sender = behind // cap
    slot = behind % cap
    delta = sender - me
    close = cells + near_buf.shape[0]
    hop = jnp.where(delta < 0, delta + PEERS, delta + PEERS - 1)
    position = jnp.where(
        v < cells,
        v,
        jnp.where(
            slot < CAP_FAR,
            close + sender * CAP_FAR + slot,
            cells + hop * rest + slot - CAP_FAR,
        ),
    )
    total = source.shape[1]
    blocks = total // 256
    for b in range(blocks):
        rel[b, :types, :] = jnp.clip(position - 256 * b, -1, 256).astype(F32)

    w = near_ref[...]
    near_rel[0, :kinds, :] = jnp.clip(w - HALO, -1, cells).astype(F32)
    near_rel[1, :kinds, :] = jnp.where(
        w < HALO, w, jnp.where(w >= HALO + cells, w - cells, -1)
    ).astype(F32)
    slips = slip_ref[...]
    for k in range(kinds):
        near_cols[k * LANES : (k + 1) * LANES, :] = mm(
            slips, one_hot(cells, near_rel[0, k : k + 1, :])
        ).astype(BF)

    group = 27

    def gather(low, count, more):
        def step(g, carry):
            for i in range(group):
                t = g * group + i
                hits = jnp.concatenate(
                    [one_hot(256, rel[low + b, pl.ds(t, 1), :]) for b in range(count)], axis=0
                )
                picked = mm(source[:, pl.ds(pl.multiple_of(low * 256, 256), count * 256)], hits).astype(BF)
                rows = pl.ds(pl.multiple_of(t * LANES, LANES), LANES)
                if more:
                    picked = picked + columns[rows, :]
                columns[rows, :] = picked
            return carry

        lax.fori_loop(0, types // group, step, 0)

    gather(0, cells // 256, False)

    leaf_cat[...] = jnp.zeros_like(leaf_cat)
    for t in range(types):
        leaf_cat[:coef, t * LANES : t * LANES + coef] = leaf_ref[t]

    for j, offset in enumerate(OFFSETS):
        @pl.when(inside(offset))
        def _():
            near_copy(j).wait_send()

        @pl.when(inside(OFFSETS[len(OFFSETS) - 1 - j]))
        def _():
            near_copy(j).wait_recv()

    source[:, cells:close] = near_buf[...].astype(F32).T.astype(BF)
    gather(cells // 256, near_buf.shape[0] // 256, True)

    for side in (0, 1):
        @pl.when(inside(1 if side else -1))
        def _():
            halo_copy(side).wait_send()

        @pl.when(inside(-1 if side else 1))
        def _():
            halo_copy(side).wait_recv()

    side_slips = jnp.concatenate(
        [halo[...], jnp.zeros((LANES - 2 * HALO, LANES), BF)], axis=0
    ).astype(F32).T.astype(BF)
    stress = jnp.zeros(out_ref.shape, F32)
    for k in range(kinds):
        column = near_cols[k * LANES : (k + 1) * LANES, :] + mm(
            side_slips, one_hot(LANES, near_rel[1, k : k + 1, :])
        ).astype(BF)
        stress = stress + mm(nb_ref[k], column)
    out_ref[...] = stress

    def wait_root(k, carry):
        root_copy(k).wait()
        return carry

    lax.fori_loop(1, n, wait_root, 0)
    base = 0
    place(base, roots[:, 0, :])
    tree_spots = []
    for bit in range(tree_bits):
        rows = n >> bit
        m, (high, low) = pair(base, rows)
        terms[spot : spot + m, :] = across(high, low)
        tree_spots.append(spot)
        spot += m
        if bit + 1 < tree_bits:
            value = lift(high, low)
            base += max(rows, 16)
            place(base, value)

    def descend(x):
        high, low = halves(x)
        return mm(high, w_down[:LANES, :]) + mm(high, w_down[LANES:, :]) + mm(low, w_down[:LANES, :])

    expansion = jnp.zeros((8, LANES), F32)
    for bit in reversed(range(tree_bits)):
        both = terms[pl.ds(tree_spots[bit] + (me >> (bit + 1)), 1), :]
        both = jnp.broadcast_to(both, (8, 2 * LANES))
        if bit + 1 < tree_bits:
            both = both + descend(expansion)
        expansion = jnp.where((me >> bit) & 1 == 0, both[:, :LANES], both[:, LANES:])
    for height in reversed(range(local_levels)):
        m = max((cells >> height) // 2, 8)
        both = descend(expansion)
        if height >= 1:
            both = both + terms[local_spots[height] : local_spots[height] + m, :]
        loc[pl.ds(0, m, stride=2), :] = both[:, :LANES]
        loc[pl.ds(1, m, stride=2), :] = both[:, LANES:]
        expansion = loc[: max(cells >> height, 8), :]

    def take_team(i, carry):
        index = mine ^ i
        start = pl.multiple_of(index * 256, 256)

        @pl.when(i == 0)
        def _():
            far_rows(start, 256 - CAP_FAR, index).wait_recv()

        @pl.when(i != 0)
        def _():
            far_rows(start, 256, index).wait_recv()

        source[:, pl.ds(close + start, 256)] = far_buf[pl.ds(start, 256), :].astype(F32).T.astype(BF)
        gather(close // 256 + index, 1, True)
        return carry

    lax.fori_loop(0, teams, take_team, 0)
    leaf_sum = mm(leaf_cat[...], columns[...])
    local_exp = (expansion.T + leaf_sum)[:coef].astype(BF)
    out_ref[...] = out_ref[...] + mm(ts_ref[...], local_exp)
    far_rows(0, (n - 1) * CAP_FAR, 0).wait_send()


def round_up(value, unit):
    return -(-value // unit) * unit


def body(*args):
    args = list(args)
    n = lax.axis_size("leaf")
    cells = args[0].shape[1]
    cap = args[8].shape[1] // n
    for i in (2, 3, 4):
        args[i] = jnp.transpose(args[i], (1, 0, 2))
    args[8] = jnp.reshape(args[8], (n, cap))
    slip, far_list, near_list = args[0], args[9], args[10]
    rest = cap - CAP_FAR
    peers = len(OFFSETS)
    total = cells + n * CAP_FAR + peers * rest
    dma = pltpu.SemaphoreType.DMA
    return pl.pallas_call(
        functools.partial(kernel, n, cells, cap),
        out_shape=pltpu.VMEM(slip.shape, F32),
        in_specs=[pl.BlockSpec(memory_space=pl.ANY)] * len(args),
        out_specs=pl.BlockSpec(memory_space=pltpu.VMEM),
        scratch_shapes=[pltpu.VMEM(a.shape, a.dtype) for a in args] + [
            pltpu.VMEM((n * CAP_FAR, LANES), BF),
            pltpu.VMEM((peers * cap, LANES), BF),
            pltpu.VMEM((n * CAP_FAR, LANES), BF),
            pltpu.VMEM((peers * rest, LANES), BF),
            pltpu.VMEM((2, HALO, LANES), BF),
            pltpu.VMEM((2 * HALO, LANES), BF),
            pltpu.VMEM((1, LANES), F32),
            pltpu.VMEM((n, 1, LANES), F32),
            pltpu.VMEM((n, cap), F32),
            pltpu.VMEM((n * CAP_FAR // LANES, LANES), F32),
            pltpu.VMEM((6, LANES, LANES), F32),
            pltpu.VMEM((2 * LANES, 2 * LANES), BF),
            pltpu.VMEM((2, 2 * LANES, 2 * LANES), BF),
            pltpu.VMEM((2 * LANES, 2 * LANES), BF),
            pltpu.VMEM((2 * cells + 2 * n + 128, LANES), F32),
            pltpu.VMEM((cells + n + 128, 2 * LANES), F32),
            pltpu.VMEM((cells, LANES), F32),
            pltpu.VMEM((total // 256, round_up(far_list.shape[0], 8), cells), F32),
            pltpu.VMEM((2, round_up(near_list.shape[0], 8), cells), F32),
            pltpu.VMEM((LANES, total), BF),
            pltpu.VMEM((LANES, far_list.shape[0] * LANES), BF),
            pltpu.VMEM((far_list.shape[0] * LANES, cells), BF),
            pltpu.VMEM((near_list.shape[0] * LANES, cells), BF),
            dma((len(args),)),
            dma,
            dma((n * CAP_FAR // 256,)),
            dma((peers,)),
            dma((peers,)),
            dma((2,)),
            dma((2,)),
            dma((n,)),
            dma((n,)),
        ],
        compiler_params=pltpu.CompilerParams(collective_id=0, has_side_effects=True),
    )(*args)


def solution(mesh):
    return jax.shard_map(
        body,
        mesh=mesh,
        in_specs=(
            P(None, "leaf"),
            P(),
            P(),
            P(),
            P(),
            P(),
            P(),
            P(),
            P("leaf", None),
            P(None, "leaf"),
            P(None, "leaf"),
        ),
        out_specs=P(None, "leaf"),
        check_vma=False,
    )
```

```python
import functools

import jax
import jax.numpy as jnp
from jax import lax
from jax.experimental import pallas as pl
from jax.experimental.pallas import tpu as pltpu
from jax.sharding import PartitionSpec as P

HALO = 32
PEERS = 4
CAP_FAR = 32
LANES = 128
BF = jnp.bfloat16
F32 = jnp.float32
MESH = pl.DeviceIdType.MESH
OFFSETS = tuple(range(-PEERS, 0)) + tuple(range(1, PEERS + 1))


def mm(a, b):
    return jnp.dot(a, b, preferred_element_type=F32)


def halves(x):
    high = x.astype(BF)
    return high, (x - high.astype(F32)).astype(BF)


def one_hot(rows, index):
    count = index.shape[1]
    lines = lax.broadcasted_iota(jnp.int32, (rows, count), 0).astype(F32).astype(BF)
    hit = lines == jnp.broadcast_to(index.astype(BF), (rows, count))
    return jnp.where(hit, jnp.ones((), BF), jnp.zeros((), BF))


def kernel(
    n, cells, cap,
    slip_any, tm_any, up_any, down_any, sib_any, leaf_any, ts_any, nb_any, send_any, far_any, near_any,
    out_ref,
    slip_ref, tm_ref, up_ref, down_ref, sib_ref, leaf_ref, ts_ref, nb_ref, send_ref, far_ref, near_ref,
    far_out, near_out, far_buf, near_buf, edges, halo, root_out, roots, send_f, far_idx,
    weight, w_up, w_sib, w_down, w_up2, w_down2, agg, terms, loc, own_loc, rel, near_rel, source, leaf_cat, columns, near_cols, load_sem,
    above, far_send, far_recv, near_send, near_recv, halo_send, halo_recv, root_send, root_recv,
):
    me = lax.axis_index("leaf")
    coef = tm_ref.shape[0]
    types = far_ref.shape[0]
    kinds = near_ref.shape[0]
    rest = cap - CAP_FAR
    team = 256 // CAP_FAR
    teams = n // team
    mine = me // team
    close = cells + near_buf.shape[0]

    pairs = (
        (slip_any, slip_ref), (tm_any, tm_ref), (send_any, send_ref), (up_any, up_ref), (sib_any, sib_ref),
        (far_any, far_ref), (near_any, near_ref), (down_any, down_ref), (leaf_any, leaf_ref), (nb_any, nb_ref),
        (ts_any, ts_ref),
    )
    loads = [pltpu.make_async_copy(a, b, load_sem.at[i]) for i, (a, b) in enumerate(pairs)]
    for copy in loads:
        copy.start()

    barrier = pltpu.get_barrier_semaphore()

    far_buf[...] = jnp.zeros_like(far_buf)
    near_buf[...] = jnp.zeros_like(near_buf)
    halo[...] = jnp.zeros_like(halo)

    def greet(q, carry):
        pl.semaphore_signal(barrier, inc=1, device_id=(q,), device_id_type=MESH)
        return carry

    lax.fori_loop(me + 1, n, greet, 0)
    @pl.when(me > 0)
    def _():
        pl.semaphore_wait(barrier, me)


    def answer(q, carry):
        pl.semaphore_signal(above.at[mine], inc=1, device_id=(q,), device_id_type=MESH)
        return carry

    lax.fori_loop(0, me, answer, 0)

    weight[...] = jnp.zeros_like(weight)
    w_sib[...] = jnp.zeros_like(w_sib)
    leaf_cat[...] = jnp.zeros_like(leaf_cat)
    for copy in loads[:3]:
        copy.wait()

    weight[0, :coef, :] = tm_ref[...].astype(F32)
    multipole = mm(weight[0].astype(BF), slip_ref[...]).astype(BF)
    source[:, :cells] = multipole
    edges[0] = slip_ref[:, :LANES].astype(F32).T[:HALO].astype(BF)
    edges[1] = slip_ref[:, cells - LANES :].astype(F32).T[LANES - HALO :].astype(BF)

    def far_copy(target):
        return pltpu.make_async_remote_copy(
            src_ref=far_out.at[pl.ds(pl.multiple_of(target * CAP_FAR, CAP_FAR), CAP_FAR)],
            dst_ref=far_buf.at[pl.ds(pl.multiple_of(me * CAP_FAR, CAP_FAR), CAP_FAR)],
            send_sem=far_send,
            recv_sem=far_recv.at[mine],
            device_id=(target,),
            device_id_type=MESH,
        )

    def far_rows(start, rows, team_index):
        return pltpu.make_async_remote_copy(
            src_ref=far_out.at[pl.ds(start, rows)],
            dst_ref=far_buf.at[pl.ds(start, rows)],
            send_sem=far_send,
            recv_sem=far_recv.at[team_index],
            device_id=(lax.rem(me + 1, n),),
            device_id_type=MESH,
        )

    def near_copy(j):
        target = jnp.clip(me + OFFSETS[j], 0, n - 1)
        back = len(OFFSETS) - 1 - j
        return pltpu.make_async_remote_copy(
            src_ref=near_out.at[pl.ds(j * cap + CAP_FAR, rest)],
            dst_ref=near_buf.at[pl.ds(back * rest, rest)],
            send_sem=near_send,
            recv_sem=near_recv,
            device_id=(target,),
            device_id_type=MESH,
        )

    def near_rows(count):
        return pltpu.make_async_remote_copy(
            src_ref=near_out.at[pl.ds(0, count * rest)],
            dst_ref=near_buf.at[pl.ds(0, count * rest)],
            send_sem=near_send,
            recv_sem=near_recv,
            device_id=(lax.rem(me + 1, n),),
            device_id_type=MESH,
        )

    def halo_copy(side):
        target = jnp.clip(me + (1 if side else -1), 0, n - 1)
        return pltpu.make_async_remote_copy(
            src_ref=edges.at[side],
            dst_ref=halo.at[pl.ds((1 - side) * HALO, HALO)],
            send_sem=halo_send.at[side],
            recv_sem=halo_recv.at[1 - side],
            device_id=(target,),
            device_id_type=MESH,
        )

    def root_copy(target):
        return pltpu.make_async_remote_copy(
            src_ref=root_out,
            dst_ref=roots.at[me],
            send_sem=root_send,
            recv_sem=root_recv,
            device_id=(target,),
            device_id_type=MESH,
        )

    def root_rows():
        return pltpu.make_async_remote_copy(
            src_ref=roots.at[pl.ds(0, n - 1)],
            dst_ref=roots.at[pl.ds(0, n - 1)],
            send_sem=root_send,
            recv_sem=root_recv,
            device_id=(lax.rem(me + 1, n),),
            device_id_type=MESH,
        )

    def inside(offset):
        return jnp.logical_and(me + offset >= 0, me + offset < n)

    send_f[...] = send_ref[...].astype(F32)
    per_row = LANES // CAP_FAR
    strip = 8 * per_row
    lane = lax.broadcasted_iota(jnp.int32, (8, LANES), 1)
    for g in range(n // strip):
        packed = send_f[pl.ds(g * strip, 8, stride=per_row), :]
        for j in range(1, per_row):
            shifted = pltpu.roll(send_f[pl.ds(g * strip + j, 8, stride=per_row), :], j * CAP_FAR, axis=1)
            packed = jnp.where(lane >= j * CAP_FAR, shifted, packed)
        far_idx[g * 8 : (g + 1) * 8, :] = packed

    def pick(first, second):
        hits = jnp.concatenate([one_hot(cells, first), one_hot(cells, second)], axis=1)
        return mm(multipole, hits).T.astype(BF)

    def pick_far(g):
        far_out[g * 256 : (g + 1) * 256, :] = pick(far_idx[2 * g : 2 * g + 1, :], far_idx[2 * g + 1 : 2 * g + 2, :])

    def pick_near(j):
        first, second = (
            send_f[pl.ds(jnp.clip(me + OFFSETS[i], 0, n - 1), 1), :] for i in (j, j + 1)
        )
        near_out[j * cap : (j + 2) * cap, :] = pick(first, second)

    for j in range(0, len(OFFSETS), 2):
        pick_near(j)

    def weave(chain, count, fillers):
        done = 0
        for i, _ in enumerate(chain):
            upto = min(len(fillers), -(-len(fillers) * (i + 1) // count))
            for work in fillers[done:upto]:
                work()
            done = upto
        for work in fillers[done:]:
            work()

    def send_far(low, high, lower):
        def step(i, carry):
            target = (i // team) * team + lax.rem(me + i, team)

            @pl.when(target < me if lower else target > me)
            def _():
                far_copy(target).start()

            return carry

        lax.fori_loop(low, high, step, 0)

    def send_near(wanted):
        for j, offset in enumerate(OFFSETS):
            if (offset < 0) == (wanted is None):
                place_of = me + offset
                ready = place_of >= 0 if wanted is None else jnp.logical_and(place_of < n, place_of // team == wanted)

                @pl.when(ready)
                def _():
                    near_copy(j).start()

    def send_root(low, high):
        def step(q, carry):
            root_copy(q).start()
            return carry

        lax.fori_loop(low, high, step, 0)

    @pl.when(inside(-1))
    def _():
        halo_copy(0).start()

    send_near(None)

    for copy in loads[3:8]:
        copy.wait()

    def parts(ref, index):
        weight[index, :coef, :coef] = ref
        weight[index, :coef, coef:] = jnp.zeros((coef, LANES - coef), F32)
        return halves(weight[index].T)

    def product(highs, lows):
        tall = [jnp.concatenate(x, axis=0) for x in (highs, lows)]
        wide = [jnp.concatenate(x, axis=1) for x in (highs, lows)]
        return halves(mm(tall[0], wide[0]) + mm(tall[0], wide[1]) + mm(tall[1], wide[0]))

    ups = [parts(up_ref[:, s, :], s) for s in (0, 1)]
    for s in (0, 1):
        w_up[s * LANES : (s + 1) * LANES, :LANES] = ups[s][0]
        w_up[s * LANES : (s + 1) * LANES, LANES:] = ups[s][1]
    for i, both in enumerate(product(*zip(*ups))):
        for c in range(4):
            w_up2[c * LANES : (c + 1) * LANES, i * LANES : (i + 1) * LANES] = both[
                (c & 1) * LANES : ((c & 1) + 1) * LANES, (c >> 1) * LANES : ((c >> 1) + 1) * LANES
            ]

    def prepare():
        for s in (0, 1):
            high, low = parts(sib_ref[:, s, :], 4 + s)
            other = 1 - s
            w_sib[0, other * LANES : (other + 1) * LANES, s * LANES : (s + 1) * LANES] = high
            w_sib[1, other * LANES : (other + 1) * LANES, s * LANES : (s + 1) * LANES] = low
        downs = [parts(down_ref[:, s, :], 2 + s) for s in (0, 1)]
        for s in (0, 1):
            w_down[:LANES, s * LANES : (s + 1) * LANES] = downs[s][0]
            w_down[LANES:, s * LANES : (s + 1) * LANES] = downs[s][1]
        for i, both in enumerate(product(*zip(*downs))):
            for s in (0, 1):
                w_down2[i * LANES : (i + 1) * LANES, 2 * s * LANES : 2 * (s + 1) * LANES] = both[
                    s * LANES : (s + 1) * LANES, :
                ]

    def pair(base, rows):
        m = max(rows // 2, 8)
        even = agg[pl.ds(base, m, stride=2), :]
        odd = agg[pl.ds(base + 1, m, stride=2), :]
        return m, halves(jnp.concatenate([even, odd], axis=1))

    def lift(base, rows):
        _, (high, low) = pair(base, rows)
        first = mm(high, w_up[...])
        second = mm(low, w_up[:, :LANES])
        return first[:, :LANES] + first[:, LANES:] + second

    def lift2(base, rows):
        m = max(rows // 4, 8)
        four = [agg[pl.ds(base + c, m, stride=4), :] for c in range(4)]
        high, low = halves(jnp.concatenate(four, axis=1))
        first = mm(high, w_up2[...])
        second = mm(low, w_up2[:, :LANES])
        return first[:, :LANES] + first[:, LANES:] + second

    def across(high, low):
        return mm(high, w_sib[0]) + mm(high, w_sib[1]) + mm(low, w_sib[0])

    def place(base, value):
        agg[base : base + value.shape[0], :] = value
        if value.shape[0] < 32:
            agg[base + value.shape[0] : base + 32, :] = jnp.zeros((32 - value.shape[0], LANES), F32)

    local_levels = cells.bit_length() - 1
    tree_bits = n.bit_length() - 1
    agg[:cells, :] = multipole.astype(F32).T
    bases = [0]
    for height in range(local_levels):
        bases.append(bases[-1] + max(cells >> height, 32))
    local_spots = [(base - cells) // 2 for base in bases]

    def spread(start, stop, spot):
        m = (stop - start) // 2
        even = agg[pl.ds(start, m, stride=2), :]
        odd = agg[pl.ds(start + 1, m, stride=2), :]
        terms[spot : spot + m, :] = across(*halves(jnp.concatenate([even, odd], axis=1)))

    def rise(bases, sizes, last):
        for height in range(0, last, 2):
            value = None
            if height + 2 <= last:
                value = lift2(bases[height], sizes[height])
                place(bases[height + 2], value)
            if height + 1 <= last:
                below = lift(bases[height], sizes[height])
                place(bases[height + 1], below)
                value = below if value is None else value
            yield value

    def climb():
        for value in rise(bases, [cells >> h for h in range(local_levels + 1)], local_levels):
            yield
        root_out[...] = value[:1]
        roots[me] = value[:1]

    def beside_own(k):
        near_cols[k * LANES : (k + 1) * LANES, :] = mm(
            slips, one_hot(cells, near_rel[0, k : k + 1, :])
        ).astype(BF)

    def column(t, starts, count, more):
        found = sum(
            mm(
                source[:, pl.ds(pl.multiple_of(low * 256, 256), count * 256)],
                jnp.concatenate([one_hot(256, rel[low + b, t : t + 1, :]) for b in range(count)], axis=0),
            )
            for low in starts
        ).astype(BF)
        if more:
            found = found + columns[t * LANES : (t + 1) * LANES, :]
        columns[t * LANES : (t + 1) * LANES, :] = found

    def columns_of(starts, count, more):
        return [functools.partial(column, t, starts, count, more) for t in range(types)]

    def gather(starts, count, more):
        for work in columns_of(starts, count, more):
            work()

    weave(
        climb(),
        (local_levels + 1) // 2,
        [functools.partial(pick_far, g) for g in range(n // (2 * per_row))],
    )

    send_root(0, me)
    send_far(0, (mine + 1) * team, True)

    @pl.when(lax.rem(me, team) < team - 1)
    def _():
        pl.semaphore_wait(above.at[mine], team - 1 - lax.rem(me, team))

    send_root(me + 1, (mine + 1) * team)
    send_near(mine)
    send_far(mine * team, (mine + 1) * team, False)

    @pl.when(mine + 1 < teams)
    def _():
        pl.semaphore_wait(above.at[mine + 1], team)
        send_root((mine + 1) * team, (mine + 2) * team)
        send_near(mine + 1)
        send_far((mine + 1) * team, (mine + 2) * team, False)

    @pl.when(inside(1))
    def _():
        halo_copy(1).start()

    for copy in loads[8:]:
        copy.wait()

    v = far_ref[...]
    behind = v - cells
    sender = behind // cap
    slot = behind % cap
    delta = sender - me
    hop = jnp.where(delta < 0, delta + PEERS, delta + PEERS - 1)
    position = jnp.where(
        v < cells,
        v,
        jnp.where(
            slot < CAP_FAR,
            close + sender * CAP_FAR + slot,
            cells + hop * rest + slot - CAP_FAR,
        ),
    )
    total = source.shape[1]
    blocks = total // 256
    for b in range(blocks):
        rel[b, :types, :] = jnp.clip(position - 256 * b, -1, 256).astype(F32)

    w = near_ref[...]
    near_rel[0, :kinds, :] = jnp.clip(w - HALO, -1, cells).astype(F32)
    near_rel[1, :kinds, :] = jnp.where(
        w < HALO, w, jnp.where(w >= HALO + cells, w - cells, -1)
    ).astype(F32)
    slips = slip_ref[...]

    def wait_team(index, own):
        start = pl.multiple_of(index * 256, 256)
        if own:
            far_rows(start, 256 - CAP_FAR, index).wait_recv()
        else:
            far_rows(start, 256, index).wait_recv()
        source[:, pl.ds(close + start, 256)] = far_buf[pl.ds(start, 256), :].astype(F32).T.astype(BF)
        return close // 256 + index

    prepare()

    def descend(x):
        high, low = halves(x)
        return mm(high, w_down[:LANES, :]) + mm(high, w_down[LANES:, :]) + mm(low, w_down[:LANES, :])

    def descend2(x):
        high, low = halves(x)
        return mm(high, w_down2[:LANES, :]) + mm(high, w_down2[LANES:, :]) + mm(low, w_down2[:LANES, :])

    def settle():
        spread(bases[1], bases[-1], 0)
        yield
        expansion = None
        for height in reversed(range(local_levels)):
            m = max((cells >> height) // 2, 8)
            both = None if expansion is None else descend(expansion)
            if height >= 1:
                term = terms[local_spots[height] : local_spots[height] + m, :]
                both = term if both is None else both + term
            own_loc[pl.ds(0, m, stride=2), :] = both[:, :LANES]
            own_loc[pl.ds(1, m, stride=2), :] = both[:, LANES:]
            expansion = own_loc[: max(cells >> height, 8), :]
            yield

    def lay(t):
        leaf_cat[:coef, t * LANES : t * LANES + coef] = leaf_ref[t]

    weave(
        settle(),
        local_levels + 1,
        columns_of([0], cells // 256, False)
        + [functools.partial(beside_own, k) for k in range(kinds)]
        + [functools.partial(lay, t) for t in range(types)],
    )

    def send_rest(index, carry):
        pl.semaphore_wait(above.at[index], team)
        send_root(index * team, (index + 1) * team)
        send_far(index * team, (index + 1) * team, False)
        return carry

    lax.fori_loop(mine + 2, teams, send_rest, 0)

    valid = jnp.minimum(me, PEERS) + jnp.minimum(n - 1 - me, PEERS)
    for count in range(PEERS, 2 * PEERS + 1):
        @pl.when(valid == count)
        def _():
            near_rows(count).wait_recv()

    source[:, cells:close] = near_buf[...].astype(F32).T.astype(BF)
    gather([cells // 256], near_buf.shape[0] // 256, True)

    for side in (0, 1):
        @pl.when(inside(-1 if side else 1))
        def _():
            halo_copy(side).wait_recv()

    side_slips = jnp.concatenate(
        [halo[...], jnp.zeros((LANES - 2 * HALO, LANES), BF)], axis=0
    ).astype(F32).T.astype(BF)
    stress = jnp.zeros(out_ref.shape, F32)
    for k in range(kinds):
        beside = near_cols[k * LANES : (k + 1) * LANES, :] + mm(
            side_slips, one_hot(LANES, near_rel[1, k : k + 1, :])
        ).astype(BF)
        stress = stress + mm(nb_ref[k], beside)
    out_ref[...] = stress

    tops = [0]
    for bit in range(tree_bits):
        tops.append(tops[-1] + max(n >> bit, 32))
    top_spot = local_spots[-1]

    def whole_tree():
        place(0, roots[:, 0, :])
        for _ in rise(tops, [n >> bit for bit in range(tree_bits)], tree_bits - 1):
            yield
        spread(0, tops[-1], top_spot)
        yield

        def chosen(bit):
            both = terms[pl.ds(top_spot + tops[bit] // 2 + (me >> (bit + 1)), 1), :]
            both = jnp.broadcast_to(both, (8, 2 * LANES))
            return jnp.where((me >> bit) & 1 == 0, both[:, :LANES], both[:, LANES:])

        def half(both, bit):
            return jnp.where((me >> bit) & 1 == 0, both[:, :LANES], both[:, LANES:])

        line = lax.broadcasted_iota(jnp.int32, (8, LANES), 0)
        expansion = chosen(tree_bits - 1)
        bit = tree_bits - 2
        if tree_bits % 2 == 0 and bit >= 0:
            expansion = half(descend(expansion), bit) + chosen(bit)
            bit -= 1
            yield
        uppers = range(bit, 0, -2)
        aside = jnp.zeros((8, LANES), F32)
        for i, k in enumerate(uppers):
            aside = jnp.where(line == i, chosen(k), aside)
        aside = descend(aside)
        for i, k in enumerate(uppers):
            quarter = descend2(expansion)
            pair_half = jnp.where((me >> k) & 1 == 0, quarter[:, : 2 * LANES], quarter[:, 2 * LANES :])
            pair_half = pair_half + jnp.broadcast_to(aside[i : i + 1, :], pair_half.shape)
            expansion = half(pair_half, k - 1) + chosen(k - 1)
            yield
        rows = 1
        if local_levels % 2:
            both = descend(expansion)
            for c in range(2):
                loc[pl.ds(c, 8, stride=2), :] = both[:, c * LANES : (c + 1) * LANES]
            rows = 2
            expansion = loc[:8, :]
            yield
        while rows < cells:
            m = max(rows, 8)
            four = descend2(expansion)
            for c in range(4):
                loc[pl.ds(c, m, stride=4), :] = four[:, c * LANES : (c + 1) * LANES]
            rows *= 4
            expansion = loc[: max(rows, 8), :]
            yield

    low = wait_team(mine, True)
    root_rows().wait_recv()
    weave(whole_tree(), tree_bits + local_levels // 2, columns_of([low], 1, True))

    def middle(i, carry):
        gather([wait_team(mine ^ i, False)], 1, True)
        return carry

    lax.fori_loop(1, teams - 1, middle, 0)

    gather([wait_team(mine ^ (teams - 1), False)], 1, True)
    leaf_sum = mm(leaf_cat[...], columns[...])
    local_exp = ((loc[...] + own_loc[...]).T + leaf_sum)[:coef].astype(BF)
    out_ref[...] = out_ref[...] + mm(ts_ref[...], local_exp)

    far_rows(0, (n - 1) * CAP_FAR, 0).wait_send()
    root_rows().wait_send()
    for count in range(PEERS, 2 * PEERS + 1):
        @pl.when(valid == count)
        def _():
            near_rows(count).wait_send()

    for side in (0, 1):
        @pl.when(inside(1 if side else -1))
        def _():
            halo_copy(side).wait_send()


def round_up(value, unit):
    return -(-value // unit) * unit


def body(*args):
    args = list(args)
    n = lax.axis_size("leaf")
    cells = args[0].shape[1]
    cap = args[8].shape[1] // n
    for i in (2, 3, 4):
        args[i] = jnp.transpose(args[i], (1, 0, 2))
    args[8] = jnp.reshape(args[8], (n, cap))
    slip, far_list, near_list = args[0], args[9], args[10]
    rest = cap - CAP_FAR
    peers = len(OFFSETS)
    total = cells + n * CAP_FAR + peers * rest
    dma = pltpu.SemaphoreType.DMA
    return pl.pallas_call(
        functools.partial(kernel, n, cells, cap),
        out_shape=pltpu.VMEM(slip.shape, F32),
        in_specs=[pl.BlockSpec(memory_space=pl.ANY)] * len(args),
        out_specs=pl.BlockSpec(memory_space=pltpu.VMEM),
        scratch_shapes=[pltpu.VMEM(a.shape, a.dtype) for a in args] + [
            pltpu.VMEM((n * CAP_FAR, LANES), BF),
            pltpu.VMEM((peers * cap, LANES), BF),
            pltpu.VMEM((n * CAP_FAR, LANES), BF),
            pltpu.VMEM((peers * rest, LANES), BF),
            pltpu.VMEM((2, HALO, LANES), BF),
            pltpu.VMEM((2 * HALO, LANES), BF),
            pltpu.VMEM((1, LANES), F32),
            pltpu.VMEM((n, 1, LANES), F32),
            pltpu.VMEM((n, cap), F32),
            pltpu.VMEM((n * CAP_FAR // LANES, LANES), F32),
            pltpu.VMEM((6, LANES, LANES), F32),
            pltpu.VMEM((2 * LANES, 2 * LANES), BF),
            pltpu.VMEM((2, 2 * LANES, 2 * LANES), BF),
            pltpu.VMEM((2 * LANES, 2 * LANES), BF),
            pltpu.VMEM((4 * LANES, 2 * LANES), BF),
            pltpu.VMEM((2 * LANES, 4 * LANES), BF),
            pltpu.VMEM((2 * cells + 2 * n + 512, LANES), F32),
            pltpu.VMEM((cells + n + 512, 2 * LANES), F32),
            pltpu.VMEM((cells, LANES), F32),
            pltpu.VMEM((cells, LANES), F32),
            pltpu.VMEM((total // 256, round_up(far_list.shape[0], 8), cells), F32),
            pltpu.VMEM((2, round_up(near_list.shape[0], 8), cells), F32),
            pltpu.VMEM((LANES, total), BF),
            pltpu.VMEM((LANES, far_list.shape[0] * LANES), BF),
            pltpu.VMEM((far_list.shape[0] * LANES, cells), BF),
            pltpu.VMEM((near_list.shape[0] * LANES, cells), BF),
            dma((len(args),)),
            pltpu.SemaphoreType.REGULAR((n * CAP_FAR // 256,)),
            dma,
            dma((n * CAP_FAR // 256,)),
            dma,
            dma,
            dma((2,)),
            dma((2,)),
            dma,
            dma,
        ],
        compiler_params=pltpu.CompilerParams(collective_id=0, has_side_effects=True),
    )(*args)


def solution(mesh):
    return jax.shard_map(
        body,
        mesh=mesh,
        in_specs=(
            P(None, "leaf"),
            P(),
            P(),
            P(),
            P(),
            P(),
            P(),
            P(),
            P("leaf", None),
            P(None, "leaf"),
            P(None, "leaf"),
        ),
        out_specs=P(None, "leaf"),
        check_vma=False,
    )
```

```python
import functools

import jax
import jax.numpy as jnp
from jax import lax
from jax.experimental import pallas as pl
from jax.experimental.pallas import tpu as pltpu
from jax.sharding import PartitionSpec as P

HALO = 32
PEERS = 4
CAP_FAR = 32
LANES = 128
BF = jnp.bfloat16
F32 = jnp.float32
MESH = pl.DeviceIdType.MESH
OFFSETS = tuple(range(-PEERS, 0)) + tuple(range(1, PEERS + 1))


def mm(a, b):
    return jnp.dot(a, b, preferred_element_type=F32)


def halves(x):
    high = x.astype(BF)
    return high, (x - high.astype(F32)).astype(BF)


def one_hot(rows, index):
    count = index.shape[1]
    lines = lax.broadcasted_iota(jnp.int32, (rows, count), 0).astype(F32).astype(BF)
    hit = lines == jnp.broadcast_to(index.astype(BF), (rows, count))
    return jnp.where(hit, jnp.ones((), BF), jnp.zeros((), BF))


def kernel(
    n, cells, cap,
    slip_any, tm_any, up_any, down_any, sib_any, leaf_any, ts_any, nb_any, send_any, far_any, near_any,
    out_ref,
    slip_ref, tm_ref, up_ref, down_ref, sib_ref, leaf_ref, ts_ref, nb_ref, send_ref, far_ref, near_ref,
    far_out, near_out, far_buf, near_buf, edges, halo, root_out, roots, send_f, far_idx,
    weight, w_up, w_sib, w_down, w_up2, w_down2, agg, terms, loc, own_loc, rel, near_rel, source, leaf_cat, columns, near_cols, load_sem,
    above, far_send, far_recv, near_send, near_recv, halo_send, halo_recv, root_send, root_recv,
):
    me = lax.axis_index("leaf")
    coef = tm_ref.shape[0]
    types = far_ref.shape[0]
    kinds = near_ref.shape[0]
    rest = cap - CAP_FAR
    team = 256 // CAP_FAR
    teams = n // team
    mine = me // team
    close = cells + near_buf.shape[0]

    pairs = (
        (slip_any, slip_ref), (tm_any, tm_ref), (send_any, send_ref), (up_any, up_ref), (sib_any, sib_ref),
        (far_any, far_ref), (near_any, near_ref), (down_any, down_ref), (leaf_any, leaf_ref), (nb_any, nb_ref),
        (ts_any, ts_ref),
    )
    loads = [pltpu.make_async_copy(a, b, load_sem.at[i]) for i, (a, b) in enumerate(pairs)]
    for copy in loads:
        copy.start()

    barrier = pltpu.get_barrier_semaphore()

    far_buf[...] = jnp.zeros_like(far_buf)
    near_buf[...] = jnp.zeros_like(near_buf)
    halo[...] = jnp.zeros_like(halo)

    def greet(q, carry):
        pl.semaphore_signal(barrier, inc=1, device_id=(q,), device_id_type=MESH)
        return carry

    lax.fori_loop(me + 1, n, greet, 0)
    @pl.when(me > 0)
    def _():
        pl.semaphore_wait(barrier, me)


    def answer(q, carry):
        pl.semaphore_signal(above.at[mine], inc=1, device_id=(q,), device_id_type=MESH)
        return carry

    lax.fori_loop(0, me, answer, 0)

    weight[...] = jnp.zeros_like(weight)
    w_sib[...] = jnp.zeros_like(w_sib)
    leaf_cat[...] = jnp.zeros_like(leaf_cat)
    for copy in loads[:3]:
        copy.wait()

    weight[0, :coef, :] = tm_ref[...].astype(F32)
    multipole = mm(weight[0].astype(BF), slip_ref[...]).astype(BF)
    source[:, :cells] = multipole
    edges[0] = slip_ref[:, :LANES].astype(F32).T[:HALO].astype(BF)
    edges[1] = slip_ref[:, cells - LANES :].astype(F32).T[LANES - HALO :].astype(BF)

    def far_copy(target):
        return pltpu.make_async_remote_copy(
            src_ref=far_out.at[pl.ds(pl.multiple_of(target * CAP_FAR, CAP_FAR), CAP_FAR)],
            dst_ref=far_buf.at[pl.ds(pl.multiple_of(me * CAP_FAR, CAP_FAR), CAP_FAR)],
            send_sem=far_send,
            recv_sem=far_recv.at[mine],
            device_id=(target,),
            device_id_type=MESH,
        )

    def far_rows(start, rows, team_index):
        return pltpu.make_async_remote_copy(
            src_ref=far_out.at[pl.ds(start, rows)],
            dst_ref=far_buf.at[pl.ds(start, rows)],
            send_sem=far_send,
            recv_sem=far_recv.at[team_index],
            device_id=(lax.rem(me + 1, n),),
            device_id_type=MESH,
        )

    def near_copy(j):
        target = jnp.clip(me + OFFSETS[j], 0, n - 1)
        back = len(OFFSETS) - 1 - j
        return pltpu.make_async_remote_copy(
            src_ref=near_out.at[pl.ds(j * cap + CAP_FAR, rest)],
            dst_ref=near_buf.at[pl.ds(back * rest, rest)],
            send_sem=near_send.at[j // PEERS],
            recv_sem=near_recv.at[back // PEERS],
            device_id=(target,),
            device_id_type=MESH,
        )

    def near_rows(side, count):
        return pltpu.make_async_remote_copy(
            src_ref=near_out.at[pl.ds(0, count * rest)],
            dst_ref=near_buf.at[pl.ds(side * PEERS * rest, count * rest)],
            send_sem=near_send.at[side],
            recv_sem=near_recv.at[side],
            device_id=(lax.rem(me + 1, n),),
            device_id_type=MESH,
        )

    def near_count(side, count):
        reach = n - 1 - me if side else me
        return reach >= count if count == PEERS else reach == count

    def halo_copy(side):
        target = jnp.clip(me + (1 if side else -1), 0, n - 1)
        return pltpu.make_async_remote_copy(
            src_ref=edges.at[side],
            dst_ref=halo.at[pl.ds((1 - side) * HALO, HALO)],
            send_sem=halo_send.at[side],
            recv_sem=halo_recv.at[1 - side],
            device_id=(target,),
            device_id_type=MESH,
        )

    def root_copy(target):
        return pltpu.make_async_remote_copy(
            src_ref=root_out,
            dst_ref=roots.at[me],
            send_sem=root_send,
            recv_sem=root_recv,
            device_id=(target,),
            device_id_type=MESH,
        )

    def root_rows():
        return pltpu.make_async_remote_copy(
            src_ref=roots.at[pl.ds(0, n - 1)],
            dst_ref=roots.at[pl.ds(0, n - 1)],
            send_sem=root_send,
            recv_sem=root_recv,
            device_id=(lax.rem(me + 1, n),),
            device_id_type=MESH,
        )

    def inside(offset):
        return jnp.logical_and(me + offset >= 0, me + offset < n)

    send_f[...] = send_ref[...].astype(F32)
    per_row = LANES // CAP_FAR
    strip = 8 * per_row
    lane = lax.broadcasted_iota(jnp.int32, (8, LANES), 1)
    for g in range(n // strip):
        packed = send_f[pl.ds(g * strip, 8, stride=per_row), :]
        for j in range(1, per_row):
            shifted = pltpu.roll(send_f[pl.ds(g * strip + j, 8, stride=per_row), :], j * CAP_FAR, axis=1)
            packed = jnp.where(lane >= j * CAP_FAR, shifted, packed)
        far_idx[g * 8 : (g + 1) * 8, :] = packed

    def pick(first, second):
        hits = jnp.concatenate([one_hot(cells, first), one_hot(cells, second)], axis=1)
        return mm(multipole, hits).T.astype(BF)

    def pick_far(g):
        far_out[g * 256 : (g + 1) * 256, :] = pick(far_idx[2 * g : 2 * g + 1, :], far_idx[2 * g + 1 : 2 * g + 2, :])

    def pick_near(j):
        first, second = (
            send_f[pl.ds(jnp.clip(me + OFFSETS[i], 0, n - 1), 1), :] for i in (j, j + 1)
        )
        near_out[j * cap : (j + 2) * cap, :] = pick(first, second)

    for j in range(0, len(OFFSETS), 2):
        pick_near(j)

    def weave(chain, count, fillers):
        done = 0
        for i, _ in enumerate(chain):
            upto = min(len(fillers), -(-len(fillers) * (i + 1) // count))
            for work in fillers[done:upto]:
                work()
            done = upto
        for work in fillers[done:]:
            work()

    def send_far(low, high, lower):
        def step(i, carry):
            target = (i // team) * team + lax.rem(me + i, team)

            @pl.when(target < me if lower else target > me)
            def _():
                far_copy(target).start()

            return carry

        lax.fori_loop(low, high, step, 0)

    def send_near(wanted):
        for j, offset in enumerate(OFFSETS):
            if (offset < 0) == (wanted is None):
                place_of = me + offset
                ready = place_of >= 0 if wanted is None else jnp.logical_and(place_of < n, place_of // team == wanted)

                @pl.when(ready)
                def _():
                    near_copy(j).start()

    def send_root(low, high):
        def step(q, carry):
            root_copy(q).start()
            return carry

        lax.fori_loop(low, high, step, 0)

    @pl.when(inside(-1))
    def _():
        halo_copy(0).start()

    send_near(None)

    for copy in loads[3:8]:
        copy.wait()

    def parts(ref, index):
        weight[index, :coef, :coef] = ref
        weight[index, :coef, coef:] = jnp.zeros((coef, LANES - coef), F32)
        return halves(weight[index].T)

    def product(highs, lows):
        tall = [jnp.concatenate(x, axis=0) for x in (highs, lows)]
        wide = [jnp.concatenate(x, axis=1) for x in (highs, lows)]
        return halves(mm(tall[0], wide[0]) + mm(tall[0], wide[1]) + mm(tall[1], wide[0]))

    ups = [parts(up_ref[:, s, :], s) for s in (0, 1)]
    for s in (0, 1):
        w_up[s * LANES : (s + 1) * LANES, :LANES] = ups[s][0]
        w_up[s * LANES : (s + 1) * LANES, LANES:] = ups[s][1]
    for i, both in enumerate(product(*zip(*ups))):
        for c in range(4):
            w_up2[c * LANES : (c + 1) * LANES, i * LANES : (i + 1) * LANES] = both[
                (c & 1) * LANES : ((c & 1) + 1) * LANES, (c >> 1) * LANES : ((c >> 1) + 1) * LANES
            ]

    def prepare():
        for s in (0, 1):
            high, low = parts(sib_ref[:, s, :], 4 + s)
            other = 1 - s
            w_sib[0, other * LANES : (other + 1) * LANES, s * LANES : (s + 1) * LANES] = high
            w_sib[1, other * LANES : (other + 1) * LANES, s * LANES : (s + 1) * LANES] = low
        downs = [parts(down_ref[:, s, :], 2 + s) for s in (0, 1)]
        for s in (0, 1):
            w_down[:LANES, s * LANES : (s + 1) * LANES] = downs[s][0]
            w_down[LANES:, s * LANES : (s + 1) * LANES] = downs[s][1]
        for i, both in enumerate(product(*zip(*downs))):
            for s in (0, 1):
                w_down2[i * LANES : (i + 1) * LANES, 2 * s * LANES : 2 * (s + 1) * LANES] = both[
                    s * LANES : (s + 1) * LANES, :
                ]

    def pair(base, rows):
        m = max(rows // 2, 8)
        even = agg[pl.ds(base, m, stride=2), :]
        odd = agg[pl.ds(base + 1, m, stride=2), :]
        return m, halves(jnp.concatenate([even, odd], axis=1))

    def lift(base, rows):
        _, (high, low) = pair(base, rows)
        first = mm(high, w_up[...])
        second = mm(low, w_up[:, :LANES])
        return first[:, :LANES] + first[:, LANES:] + second

    def lift2(base, rows):
        m = max(rows // 4, 8)
        four = [agg[pl.ds(base + c, m, stride=4), :] for c in range(4)]
        high, low = halves(jnp.concatenate(four, axis=1))
        first = mm(high, w_up2[...])
        second = mm(low, w_up2[:, :LANES])
        return first[:, :LANES] + first[:, LANES:] + second

    def across(high, low):
        return mm(high, w_sib[0]) + mm(high, w_sib[1]) + mm(low, w_sib[0])

    def place(base, value):
        agg[base : base + value.shape[0], :] = value
        if value.shape[0] < 32:
            agg[base + value.shape[0] : base + 32, :] = jnp.zeros((32 - value.shape[0], LANES), F32)

    local_levels = cells.bit_length() - 1
    tree_bits = n.bit_length() - 1
    agg[:cells, :] = multipole.astype(F32).T
    bases = [0]
    for height in range(local_levels):
        bases.append(bases[-1] + max(cells >> height, 32))
    local_spots = [(base - cells) // 2 for base in bases]

    def spread(start, stop, spot):
        m = (stop - start) // 2
        even = agg[pl.ds(start, m, stride=2), :]
        odd = agg[pl.ds(start + 1, m, stride=2), :]
        terms[spot : spot + m, :] = across(*halves(jnp.concatenate([even, odd], axis=1)))

    def rise(bases, sizes, last):
        for height in range(0, last, 2):
            value = None
            if height + 2 <= last:
                value = lift2(bases[height], sizes[height])
                place(bases[height + 2], value)
            if height + 1 <= last:
                below = lift(bases[height], sizes[height])
                place(bases[height + 1], below)
                value = below if value is None else value
            yield value

    def climb():
        for value in rise(bases, [cells >> h for h in range(local_levels + 1)], local_levels):
            yield
        root_out[...] = value[:1]
        roots[me] = value[:1]

    def beside_own(k):
        near_cols[k * LANES : (k + 1) * LANES, :] = mm(
            slips, one_hot(cells, near_rel[0, k : k + 1, :])
        ).astype(BF)

    def column(t, starts, count, more):
        found = sum(
            mm(
                source[:, pl.ds(pl.multiple_of(low * 256, 256), count * 256)],
                jnp.concatenate([one_hot(256, rel[low + b, t : t + 1, :]) for b in range(count)], axis=0),
            )
            for low in starts
        ).astype(BF)
        if more:
            found = found + columns[t * LANES : (t + 1) * LANES, :]
        columns[t * LANES : (t + 1) * LANES, :] = found

    def columns_of(starts, count, more):
        return [functools.partial(column, t, starts, count, more) for t in range(types)]

    def gather(starts, count, more):
        for work in columns_of(starts, count, more):
            work()

    weave(
        climb(),
        (local_levels + 1) // 2,
        [functools.partial(pick_far, g) for g in range(n // (2 * per_row))],
    )

    send_root(0, me)

    @pl.when(lax.rem(me, team) < team - 1)
    def _():
        pl.semaphore_wait(above.at[mine], team - 1 - lax.rem(me, team))
        halo_copy(1).start()

    send_root(me + 1, (mine + 1) * team)
    send_near(mine)

    @pl.when(mine + 1 < teams)
    def _():
        pl.semaphore_wait(above.at[mine + 1], team)

        @pl.when(lax.rem(me, team) == team - 1)
        def _():
            halo_copy(1).start()

        send_near(mine + 1)
        send_root((mine + 1) * team, (mine + 2) * team)

    send_far(0, (mine + 1) * team, True)
    send_far(mine * team, (mine + 1) * team, False)

    for copy in loads[8:]:
        copy.wait()

    v = far_ref[...]
    behind = v - cells
    sender = behind // cap
    slot = behind % cap
    delta = sender - me
    hop = jnp.where(delta < 0, delta + PEERS, delta + PEERS - 1)
    position = jnp.where(
        v < cells,
        v,
        jnp.where(
            slot < CAP_FAR,
            close + sender * CAP_FAR + slot,
            cells + hop * rest + slot - CAP_FAR,
        ),
    )
    total = source.shape[1]
    blocks = total // 256
    for b in range(blocks):
        rel[b, :types, :] = jnp.clip(position - 256 * b, -1, 256).astype(F32)

    w = near_ref[...]
    near_rel[0, :kinds, :] = jnp.clip(w - HALO, -1, cells).astype(F32)
    near_rel[1, :kinds, :] = jnp.where(
        w < HALO, w, jnp.where(w >= HALO + cells, w - cells, -1)
    ).astype(F32)
    slips = slip_ref[...]

    def wait_team(index, own):
        start = pl.multiple_of(index * 256, 256)
        if own:
            far_rows(start, 256 - CAP_FAR, index).wait_recv()
        else:
            far_rows(start, 256, index).wait_recv()
        source[:, pl.ds(close + start, 256)] = far_buf[pl.ds(start, 256), :].astype(F32).T.astype(BF)
        return close // 256 + index

    prepare()

    def descend(x):
        high, low = halves(x)
        return mm(high, w_down[:LANES, :]) + mm(high, w_down[LANES:, :]) + mm(low, w_down[:LANES, :])

    def descend2(x):
        high, low = halves(x)
        return mm(high, w_down2[:LANES, :]) + mm(high, w_down2[LANES:, :]) + mm(low, w_down2[:LANES, :])

    def settle():
        spread(bases[1], bases[-1], 0)
        yield
        expansion = None
        for height in reversed(range(local_levels)):
            m = max((cells >> height) // 2, 8)
            both = None if expansion is None else descend(expansion)
            if height >= 1:
                term = terms[local_spots[height] : local_spots[height] + m, :]
                both = term if both is None else both + term
            own_loc[pl.ds(0, m, stride=2), :] = both[:, :LANES]
            own_loc[pl.ds(1, m, stride=2), :] = both[:, LANES:]
            expansion = own_loc[: max(cells >> height, 8), :]
            yield

    def lay(t):
        leaf_cat[:coef, t * LANES : t * LANES + coef] = leaf_ref[t]

    weave(
        settle(),
        local_levels + 1,
        columns_of([0], cells // 256, False)
        + [functools.partial(beside_own, k) for k in range(kinds)]
        + [functools.partial(lay, t) for t in range(types)],
    )


    def send_rest(index, carry):
        pl.semaphore_wait(above.at[index], team)
        send_root(index * team, (index + 1) * team)
        return carry

    lax.fori_loop(mine + 2, teams, send_rest, 0)
    send_far((mine + 1) * team, n, False)

    def wait_near(side):
        for count in range(1, PEERS + 1):
            @pl.when(near_count(side, count))
            def _():
                near_rows(side, count).wait_recv()

    def land_near(side):
        start, rows = side * PEERS * rest, PEERS * rest
        source[:, cells + start : cells + start + rows] = near_buf[start : start + rows, :].astype(F32).T.astype(BF)

    def near_column(side, t):
        start = cells + side * PEERS * rest
        stop = start + PEERS * rest
        hits = []
        at = start
        while at < stop:
            block, skip = divmod(at, 256)
            size = min(256 - skip, stop - at)
            index = rel[block, t : t + 1, :]
            hits.append(one_hot(size, index - skip if skip else index))
            at += size
        found = mm(source[:, start:stop], jnp.concatenate(hits, axis=0)).astype(BF)
        columns[t * LANES : (t + 1) * LANES, :] = found + columns[t * LANES : (t + 1) * LANES, :]

    wait_near(1)
    land_near(1)
    for t in range(types):
        near_column(1, t)

    wait_near(0)
    for side in (0, 1):
        @pl.when(inside(-1 if side else 1))
        def _():
            halo_copy(side).wait_recv()

    land_near(0)
    side_slips = jnp.concatenate(
        [halo[...], jnp.zeros((LANES - 2 * HALO, LANES), BF)], axis=0
    ).astype(F32).T.astype(BF)
    stress = jnp.zeros(out_ref.shape, F32)
    for k in range(kinds):
        beside = near_cols[k * LANES : (k + 1) * LANES, :] + mm(
            side_slips, one_hot(LANES, near_rel[1, k : k + 1, :])
        ).astype(BF)
        stress = stress + mm(nb_ref[k], beside)
    out_ref[...] = stress
    for t in range(types):
        near_column(0, t)

    tops = [0]
    for bit in range(tree_bits):
        tops.append(tops[-1] + max(n >> bit, 32))
    top_spot = local_spots[-1]

    def whole_tree():
        place(0, roots[:, 0, :])
        for _ in rise(tops, [n >> bit for bit in range(tree_bits)], tree_bits - 1):
            yield
        spread(0, tops[-1], top_spot)
        yield

        def chosen(bit):
            both = terms[pl.ds(top_spot + tops[bit] // 2 + (me >> (bit + 1)), 1), :]
            both = jnp.broadcast_to(both, (8, 2 * LANES))
            return jnp.where((me >> bit) & 1 == 0, both[:, :LANES], both[:, LANES:])

        def half(both, bit):
            return jnp.where((me >> bit) & 1 == 0, both[:, :LANES], both[:, LANES:])

        line = lax.broadcasted_iota(jnp.int32, (8, LANES), 0)
        expansion = chosen(tree_bits - 1)
        bit = tree_bits - 2
        if tree_bits % 2 == 0 and bit >= 0:
            expansion = half(descend(expansion), bit) + chosen(bit)
            bit -= 1
            yield
        uppers = range(bit, 0, -2)
        aside = jnp.zeros((8, LANES), F32)
        for i, k in enumerate(uppers):
            aside = jnp.where(line == i, chosen(k), aside)
        aside = descend(aside)
        for i, k in enumerate(uppers):
            quarter = descend2(expansion)
            pair_half = jnp.where((me >> k) & 1 == 0, quarter[:, : 2 * LANES], quarter[:, 2 * LANES :])
            pair_half = pair_half + jnp.broadcast_to(aside[i : i + 1, :], pair_half.shape)
            expansion = half(pair_half, k - 1) + chosen(k - 1)
            yield
        rows = 1
        if local_levels % 2:
            both = descend(expansion)
            for c in range(2):
                loc[pl.ds(c, 8, stride=2), :] = both[:, c * LANES : (c + 1) * LANES]
            rows = 2
            expansion = loc[:8, :]
            yield
        while rows < cells:
            m = max(rows, 8)
            four = descend2(expansion)
            for c in range(4):
                loc[pl.ds(c, m, stride=4), :] = four[:, c * LANES : (c + 1) * LANES]
            rows *= 4
            expansion = loc[: max(rows, 8), :]
            yield

    root_rows().wait_recv()
    weave(
        whole_tree(),
        tree_bits + local_levels // 2,
        columns_of([wait_team(mine, True), wait_team(mine ^ 1, False)], 1, True),
    )

    def finish(low, following):
        works = columns_of([low], 1, True)
        cut = types // 2
        for work in works[:cut]:
            work()
        low = None if following is None else wait_team(following, False)
        for work in works[cut:]:
            work()
        return low

    if teams <= 4:
        low = wait_team(mine ^ 2, False)
        for i in range(3, teams):
            low = finish(low, mine ^ i)
        finish(low, None)
    else:
        def middle(i, carry):
            gather([wait_team(mine ^ i, False)], 1, True)
            return carry

        lax.fori_loop(2, teams, middle, 0)

    leaf_sum = mm(leaf_cat[...], columns[...])
    local_exp = ((loc[...] + own_loc[...]).T + leaf_sum)[:coef].astype(BF)
    out_ref[...] = out_ref[...] + mm(ts_ref[...], local_exp)

    far_rows(0, (n - 1) * CAP_FAR, 0).wait_send()
    root_rows().wait_send()
    for side in (0, 1):
        for count in range(1, PEERS + 1):
            @pl.when(near_count(side, count))
            def _():
                near_rows(side, count).wait_send()

    for side in (0, 1):
        @pl.when(inside(1 if side else -1))
        def _():
            halo_copy(side).wait_send()


def round_up(value, unit):
    return -(-value // unit) * unit


def body(*args):
    args = list(args)
    n = lax.axis_size("leaf")
    cells = args[0].shape[1]
    cap = args[8].shape[1] // n
    for i in (2, 3, 4):
        args[i] = jnp.transpose(args[i], (1, 0, 2))
    args[8] = jnp.reshape(args[8], (n, cap))
    slip, far_list, near_list = args[0], args[9], args[10]
    rest = cap - CAP_FAR
    peers = len(OFFSETS)
    total = cells + n * CAP_FAR + peers * rest
    dma = pltpu.SemaphoreType.DMA
    return pl.pallas_call(
        functools.partial(kernel, n, cells, cap),
        out_shape=pltpu.VMEM(slip.shape, F32),
        in_specs=[pl.BlockSpec(memory_space=pl.ANY)] * len(args),
        out_specs=pl.BlockSpec(memory_space=pltpu.VMEM),
        scratch_shapes=[pltpu.VMEM(a.shape, a.dtype) for a in args] + [
            pltpu.VMEM((n * CAP_FAR, LANES), BF),
            pltpu.VMEM((peers * cap, LANES), BF),
            pltpu.VMEM((n * CAP_FAR, LANES), BF),
            pltpu.VMEM((peers * rest, LANES), BF),
            pltpu.VMEM((2, HALO, LANES), BF),
            pltpu.VMEM((2 * HALO, LANES), BF),
            pltpu.VMEM((1, LANES), F32),
            pltpu.VMEM((n, 1, LANES), F32),
            pltpu.VMEM((n, cap), F32),
            pltpu.VMEM((n * CAP_FAR // LANES, LANES), F32),
            pltpu.VMEM((6, LANES, LANES), F32),
            pltpu.VMEM((2 * LANES, 2 * LANES), BF),
            pltpu.VMEM((2, 2 * LANES, 2 * LANES), BF),
            pltpu.VMEM((2 * LANES, 2 * LANES), BF),
            pltpu.VMEM((4 * LANES, 2 * LANES), BF),
            pltpu.VMEM((2 * LANES, 4 * LANES), BF),
            pltpu.VMEM((2 * cells + 2 * n + 512, LANES), F32),
            pltpu.VMEM((cells + n + 512, 2 * LANES), F32),
            pltpu.VMEM((cells, LANES), F32),
            pltpu.VMEM((cells, LANES), F32),
            pltpu.VMEM((total // 256, round_up(far_list.shape[0], 8), cells), F32),
            pltpu.VMEM((2, round_up(near_list.shape[0], 8), cells), F32),
            pltpu.VMEM((LANES, total), BF),
            pltpu.VMEM((LANES, far_list.shape[0] * LANES), BF),
            pltpu.VMEM((far_list.shape[0] * LANES, cells), BF),
            pltpu.VMEM((near_list.shape[0] * LANES, cells), BF),
            dma((len(args),)),
            pltpu.SemaphoreType.REGULAR((n * CAP_FAR // 256,)),
            dma,
            dma((n * CAP_FAR // 256,)),
            dma((2,)),
            dma((2,)),
            dma((2,)),
            dma((2,)),
            dma,
            dma,
        ],
        compiler_params=pltpu.CompilerParams(collective_id=0, has_side_effects=True),
    )(*args)


def solution(mesh):
    return jax.shard_map(
        body,
        mesh=mesh,
        in_specs=(
            P(None, "leaf"),
            P(),
            P(),
            P(),
            P(),
            P(),
            P(),
            P(),
            P("leaf", None),
            P(None, "leaf"),
            P(None, "leaf"),
        ),
        out_specs=P(None, "leaf"),
        check_vma=False,
    )
```

```python
import functools

import jax
import jax.numpy as jnp
from jax import lax
from jax.experimental import pallas as pl
from jax.experimental.pallas import tpu as pltpu
from jax.sharding import PartitionSpec as P

HALO = 32
PEERS = 4
CAP_FAR = 32
LANES = 128
BF = jnp.bfloat16
F32 = jnp.float32
MESH = pl.DeviceIdType.MESH
OFFSETS = tuple(range(-PEERS, 0)) + tuple(range(1, PEERS + 1))


def mm(a, b):
    return jnp.dot(a, b, preferred_element_type=F32)


def halves(x):
    high = x.astype(BF)
    return high, (x - high.astype(F32)).astype(BF)


def one_hot(rows, index):
    count = index.shape[1]
    lines = lax.broadcasted_iota(jnp.int32, (rows, count), 0).astype(F32).astype(BF)
    hit = lines == jnp.broadcast_to(index.astype(BF), (rows, count))
    return jnp.where(hit, jnp.ones((), BF), jnp.zeros((), BF))


def kernel(
    n, cells, cap,
    slip_any, tm_any, up_any, down_any, sib_any, leaf_any, ts_any, nb_any, send_any, far_any, near_any,
    out_ref,
    slip_ref, tm_ref, up_ref, down_ref, sib_ref, leaf_ref, ts_ref, nb_ref, send_ref, far_ref, near_ref,
    far_out, near_out, far_buf, near_buf, edges, halo, root_out, roots, send_f, far_idx,
    weight, w_up, w_sib, w_down, w_up2, w_down2, agg, terms, loc, own_loc, rel, near_rel, source, leaf_cat, columns, near_cols, load_sem,
    above, far_send, far_recv, near_send, near_recv, halo_send, halo_recv, root_send, root_recv,
):
    me = lax.axis_index("leaf")
    coef = tm_ref.shape[0]
    types = far_ref.shape[0]
    kinds = near_ref.shape[0]
    rest = cap - CAP_FAR
    team = 256 // CAP_FAR
    teams = n // team
    mine = me // team
    close = cells + near_buf.shape[0]

    pairs = (
        (slip_any, slip_ref), (tm_any, tm_ref), (send_any, send_ref), (up_any, up_ref), (sib_any, sib_ref),
        (far_any, far_ref), (near_any, near_ref), (down_any, down_ref), (leaf_any, leaf_ref), (nb_any, nb_ref),
        (ts_any, ts_ref),
    )
    loads = [pltpu.make_async_copy(a, b, load_sem.at[i]) for i, (a, b) in enumerate(pairs)]
    for copy in loads:
        copy.start()

    barrier = pltpu.get_barrier_semaphore()

    far_buf[...] = jnp.zeros_like(far_buf)
    near_buf[...] = jnp.zeros_like(near_buf)
    halo[...] = jnp.zeros_like(halo)

    def greet(q, carry):
        pl.semaphore_signal(barrier, inc=1, device_id=(q,), device_id_type=MESH)
        return carry

    lax.fori_loop(me + 1, n, greet, 0)
    def answer(q, carry):
        pl.semaphore_signal(above.at[mine], inc=1, device_id=(q,), device_id_type=MESH)
        return carry

    weight[...] = jnp.zeros_like(weight)
    w_sib[...] = jnp.zeros_like(w_sib)
    leaf_cat[...] = jnp.zeros_like(leaf_cat)
    for copy in loads[:3]:
        copy.wait()

    weight[0, :coef, :] = tm_ref[...].astype(F32)
    multipole = mm(weight[0].astype(BF), slip_ref[...]).astype(BF)
    source[:, :cells] = multipole
    edges[0] = slip_ref[:, :LANES].astype(F32).T[:HALO].astype(BF)
    edges[1] = slip_ref[:, cells - LANES :].astype(F32).T[LANES - HALO :].astype(BF)

    def far_copy(target):
        return pltpu.make_async_remote_copy(
            src_ref=far_out.at[pl.ds(pl.multiple_of(target * CAP_FAR, CAP_FAR), CAP_FAR)],
            dst_ref=far_buf.at[pl.ds(pl.multiple_of(me * CAP_FAR, CAP_FAR), CAP_FAR)],
            send_sem=far_send,
            recv_sem=far_recv.at[mine],
            device_id=(target,),
            device_id_type=MESH,
        )

    def far_rows(start, rows, team_index):
        return pltpu.make_async_remote_copy(
            src_ref=far_out.at[pl.ds(start, rows)],
            dst_ref=far_buf.at[pl.ds(start, rows)],
            send_sem=far_send,
            recv_sem=far_recv.at[team_index],
            device_id=(lax.rem(me + 1, n),),
            device_id_type=MESH,
        )

    def near_copy(j):
        target = jnp.clip(me + OFFSETS[j], 0, n - 1)
        back = len(OFFSETS) - 1 - j
        return pltpu.make_async_remote_copy(
            src_ref=near_out.at[pl.ds(j * cap + CAP_FAR, rest)],
            dst_ref=near_buf.at[pl.ds(back * rest, rest)],
            send_sem=near_send.at[j // PEERS],
            recv_sem=near_recv.at[back // PEERS],
            device_id=(target,),
            device_id_type=MESH,
        )

    def near_rows(side, count):
        return pltpu.make_async_remote_copy(
            src_ref=near_out.at[pl.ds(0, count * rest)],
            dst_ref=near_buf.at[pl.ds(side * PEERS * rest, count * rest)],
            send_sem=near_send.at[side],
            recv_sem=near_recv.at[side],
            device_id=(lax.rem(me + 1, n),),
            device_id_type=MESH,
        )

    def near_count(side, count):
        reach = n - 1 - me if side else me
        return reach >= count if count == PEERS else reach == count

    def halo_copy(side):
        target = jnp.clip(me + (1 if side else -1), 0, n - 1)
        return pltpu.make_async_remote_copy(
            src_ref=edges.at[side],
            dst_ref=halo.at[pl.ds((1 - side) * HALO, HALO)],
            send_sem=halo_send.at[side],
            recv_sem=halo_recv.at[1 - side],
            device_id=(target,),
            device_id_type=MESH,
        )

    def root_copy(target):
        return pltpu.make_async_remote_copy(
            src_ref=root_out,
            dst_ref=roots.at[me],
            send_sem=root_send,
            recv_sem=root_recv,
            device_id=(target,),
            device_id_type=MESH,
        )

    def root_rows():
        return pltpu.make_async_remote_copy(
            src_ref=roots.at[pl.ds(0, n - 1)],
            dst_ref=roots.at[pl.ds(0, n - 1)],
            send_sem=root_send,
            recv_sem=root_recv,
            device_id=(lax.rem(me + 1, n),),
            device_id_type=MESH,
        )

    def inside(offset):
        return jnp.logical_and(me + offset >= 0, me + offset < n)

    send_f[...] = send_ref[...].astype(F32)
    per_row = LANES // CAP_FAR
    strip = 8 * per_row
    lane = lax.broadcasted_iota(jnp.int32, (8, LANES), 1)
    for g in range(n // strip):
        packed = send_f[pl.ds(g * strip, 8, stride=per_row), :]
        for j in range(1, per_row):
            shifted = pltpu.roll(send_f[pl.ds(g * strip + j, 8, stride=per_row), :], j * CAP_FAR, axis=1)
            packed = jnp.where(lane >= j * CAP_FAR, shifted, packed)
        far_idx[g * 8 : (g + 1) * 8, :] = packed

    def pick(first, second):
        hits = jnp.concatenate([one_hot(cells, first), one_hot(cells, second)], axis=1)
        return mm(multipole, hits).T.astype(BF)

    def pick_far(g):
        far_out[g * 256 : (g + 1) * 256, :] = pick(far_idx[2 * g : 2 * g + 1, :], far_idx[2 * g + 1 : 2 * g + 2, :])

    def pick_near(j):
        first, second = (
            send_f[pl.ds(jnp.clip(me + OFFSETS[i], 0, n - 1), 1), :] for i in (j, j + 1)
        )
        near_out[j * cap : (j + 2) * cap, :] = pick(first, second)

    for j in range(0, len(OFFSETS), 2):
        pick_near(j)

    def weave(chain, count, fillers):
        done = 0
        for i, _ in enumerate(chain):
            upto = min(len(fillers), -(-len(fillers) * (i + 1) // count))
            for work in fillers[done:upto]:
                work()
            done = upto
        for work in fillers[done:]:
            work()

    def send_far(low, high, lower):
        def step(i, carry):
            group = i // team if lower else jnp.where(mine == 0, lax.rem(i // team, teams), mine + teams - i // team)
            target = group * team + lax.rem(me + i, team)

            @pl.when(target < me if lower else target > me)
            def _():
                far_copy(target).start()

            return carry

        lax.fori_loop(low, high, step, 0)

    def send_near(wanted):
        for j, offset in enumerate(OFFSETS):
            if (offset < 0) == (wanted is None):
                place_of = me + offset
                ready = place_of >= 0 if wanted is None else jnp.logical_and(place_of < n, place_of // team == wanted)

                @pl.when(ready)
                def _():
                    near_copy(j).start()

    def send_root(low, high):
        def step(q, carry):
            root_copy(q).start()
            return carry

        lax.fori_loop(low, high, step, 0)

    def first_sends():
        @pl.when(me > 0)
        def _():
            pl.semaphore_wait(barrier, me)
            halo_copy(0).start()

        lax.fori_loop(0, me, answer, 0)
        send_near(None)

    late = lax.rem(me, team) < 2

    @pl.when(jnp.logical_not(late))
    def _():
        first_sends()

    for copy in loads[3:8]:
        copy.wait()

    def parts(ref, index):
        weight[index, :coef, :coef] = ref
        weight[index, :coef, coef:] = jnp.zeros((coef, LANES - coef), F32)
        return halves(weight[index].T)

    def product(highs, lows):
        tall = [jnp.concatenate(x, axis=0) for x in (highs, lows)]
        wide = [jnp.concatenate(x, axis=1) for x in (highs, lows)]
        return halves(mm(tall[0], wide[0]) + mm(tall[0], wide[1]) + mm(tall[1], wide[0]))

    ups = [parts(up_ref[:, s, :], s) for s in (0, 1)]
    for s in (0, 1):
        w_up[s * LANES : (s + 1) * LANES, :LANES] = ups[s][0]
        w_up[s * LANES : (s + 1) * LANES, LANES:] = ups[s][1]
    for i, both in enumerate(product(*zip(*ups))):
        for c in range(4):
            w_up2[c * LANES : (c + 1) * LANES, i * LANES : (i + 1) * LANES] = both[
                (c & 1) * LANES : ((c & 1) + 1) * LANES, (c >> 1) * LANES : ((c >> 1) + 1) * LANES
            ]

    def prepare():
        for s in (0, 1):
            high, low = parts(sib_ref[:, s, :], 4 + s)
            other = 1 - s
            w_sib[0, other * LANES : (other + 1) * LANES, s * LANES : (s + 1) * LANES] = high
            w_sib[1, other * LANES : (other + 1) * LANES, s * LANES : (s + 1) * LANES] = low
        downs = [parts(down_ref[:, s, :], 2 + s) for s in (0, 1)]
        for s in (0, 1):
            w_down[:LANES, s * LANES : (s + 1) * LANES] = downs[s][0]
            w_down[LANES:, s * LANES : (s + 1) * LANES] = downs[s][1]
        for i, both in enumerate(product(*zip(*downs))):
            for s in (0, 1):
                w_down2[i * LANES : (i + 1) * LANES, 2 * s * LANES : 2 * (s + 1) * LANES] = both[
                    s * LANES : (s + 1) * LANES, :
                ]

    def pair(base, rows):
        m = max(rows // 2, 8)
        even = agg[pl.ds(base, m, stride=2), :]
        odd = agg[pl.ds(base + 1, m, stride=2), :]
        return m, halves(jnp.concatenate([even, odd], axis=1))

    def lift(base, rows):
        _, (high, low) = pair(base, rows)
        first = mm(high, w_up[...])
        second = mm(low, w_up[:, :LANES])
        return first[:, :LANES] + first[:, LANES:] + second

    def lift2(base, rows):
        m = max(rows // 4, 8)
        four = [agg[pl.ds(base + c, m, stride=4), :] for c in range(4)]
        high, low = halves(jnp.concatenate(four, axis=1))
        first = mm(high, w_up2[...])
        second = mm(low, w_up2[:, :LANES])
        return first[:, :LANES] + first[:, LANES:] + second

    def across(high, low):
        return mm(high, w_sib[0]) + mm(high, w_sib[1]) + mm(low, w_sib[0])

    def place(base, value):
        agg[base : base + value.shape[0], :] = value
        if value.shape[0] < 32:
            agg[base + value.shape[0] : base + 32, :] = jnp.zeros((32 - value.shape[0], LANES), F32)

    local_levels = cells.bit_length() - 1
    tree_bits = n.bit_length() - 1
    agg[:cells, :] = multipole.astype(F32).T
    bases = [0]
    for height in range(local_levels):
        bases.append(bases[-1] + max(cells >> height, 32))
    local_spots = [(base - cells) // 2 for base in bases]

    def spread(start, stop, spot):
        m = (stop - start) // 2
        even = agg[pl.ds(start, m, stride=2), :]
        odd = agg[pl.ds(start + 1, m, stride=2), :]
        terms[spot : spot + m, :] = across(*halves(jnp.concatenate([even, odd], axis=1)))

    def rise(bases, sizes, last):
        for height in range(0, last, 2):
            value = None
            if height + 2 <= last:
                value = lift2(bases[height], sizes[height])
                place(bases[height + 2], value)
            if height + 1 <= last:
                below = lift(bases[height], sizes[height])
                place(bases[height + 1], below)
                value = below if value is None else value
            yield value

    def climb():
        for value in rise(bases, [cells >> h for h in range(local_levels + 1)], local_levels):
            yield
        root_out[...] = value[:1]
        roots[me] = value[:1]

    def beside_own(k):
        near_cols[k * LANES : (k + 1) * LANES, :] = mm(
            slips, one_hot(cells, near_rel[0, k : k + 1, :])
        ).astype(BF)

    def column(t, starts, count, more):
        found = sum(
            mm(
                source[:, pl.ds(pl.multiple_of(low * 256, 256), count * 256)],
                jnp.concatenate([one_hot(256, rel[low + b, t : t + 1, :]) for b in range(count)], axis=0),
            )
            for low in starts
        ).astype(BF)
        if more:
            found = found + columns[t * LANES : (t + 1) * LANES, :]
        columns[t * LANES : (t + 1) * LANES, :] = found

    def columns_of(starts, count, more):
        return [functools.partial(column, t, starts, count, more) for t in range(types)]

    def gather(starts, count, more):
        for work in columns_of(starts, count, more):
            work()

    weave(
        climb(),
        (local_levels + 1) // 2,
        [functools.partial(pick_far, g) for g in range(n // (2 * per_row))],
    )

    @pl.when(late)
    def _():
        first_sends()

    send_root(0, me)

    @pl.when(mine > 0)
    def _():
        send_far(0, team, True)

    @pl.when(lax.rem(me, team) < team - 1)
    def _():
        pl.semaphore_wait(above.at[mine], team - 1 - lax.rem(me, team))
        halo_copy(1).start()

    send_root(me + 1, (mine + 1) * team)
    send_near(mine)

    @pl.when(mine + 1 < teams)
    def _():
        pl.semaphore_wait(above.at[mine + 1], team)

        @pl.when(lax.rem(me, team) == team - 1)
        def _():
            halo_copy(1).start()

        send_near(mine + 1)
        send_root((mine + 1) * team, (mine + 2) * team)

    send_far(jnp.minimum(mine, 1) * team, (mine + 1) * team, True)
    send_far(n, n + team, False)

    for copy in loads[8:]:
        copy.wait()

    v = far_ref[...]
    behind = v - cells
    sender = behind // cap
    slot = behind % cap
    delta = sender - me
    hop = jnp.where(delta < 0, delta + PEERS, delta + PEERS - 1)
    position = jnp.where(
        v < cells,
        v,
        jnp.where(
            slot < CAP_FAR,
            close + sender * CAP_FAR + slot,
            cells + hop * rest + slot - CAP_FAR,
        ),
    )
    total = source.shape[1]
    blocks = total // 256
    for b in range(blocks):
        rel[b, :types, :] = jnp.clip(position - 256 * b, -1, 256).astype(F32)

    w = near_ref[...]
    near_rel[0, :kinds, :] = jnp.clip(w - HALO, -1, cells).astype(F32)
    near_rel[1, :kinds, :] = jnp.where(
        w < HALO, w, jnp.where(w >= HALO + cells, w - cells, -1)
    ).astype(F32)
    slips = slip_ref[...]

    def wait_team(index, own):
        start = pl.multiple_of(index * 256, 256)
        if own:
            far_rows(start, 256 - CAP_FAR, index).wait_recv()
        else:
            far_rows(start, 256, index).wait_recv()
        source[:, pl.ds(close + start, 256)] = far_buf[pl.ds(start, 256), :].astype(F32).T.astype(BF)
        return close // 256 + index

    prepare()

    def descend(x):
        high, low = halves(x)
        return mm(high, w_down[:LANES, :]) + mm(high, w_down[LANES:, :]) + mm(low, w_down[:LANES, :])

    def descend2(x):
        high, low = halves(x)
        return mm(high, w_down2[:LANES, :]) + mm(high, w_down2[LANES:, :]) + mm(low, w_down2[:LANES, :])

    def settle():
        spread(bases[1], bases[-1], 0)
        yield
        expansion = None
        for height in reversed(range(local_levels)):
            m = max((cells >> height) // 2, 8)
            both = None if expansion is None else descend(expansion)
            if height >= 1:
                term = terms[local_spots[height] : local_spots[height] + m, :]
                both = term if both is None else both + term
            own_loc[pl.ds(0, m, stride=2), :] = both[:, :LANES]
            own_loc[pl.ds(1, m, stride=2), :] = both[:, LANES:]
            expansion = own_loc[: max(cells >> height, 8), :]
            yield

    def lay(t):
        leaf_cat[:coef, t * LANES : t * LANES + coef] = leaf_ref[t]

    def own_work():
        weave(
            settle(),
            local_levels + 1,
            columns_of([0], cells // 256, False)
            + [functools.partial(beside_own, k) for k in range(kinds)]
            + [functools.partial(lay, t) for t in range(types)],
        )

    @pl.when(mine == 0)
    def _():
        own_work()

    def send_rest(index, carry):
        pl.semaphore_wait(above.at[index], team)
        send_root(index * team, (index + 1) * team)
        return carry

    lax.fori_loop(mine + 2, teams, send_rest, 0)
    send_far((mine + 1) * team, n, False)

    @pl.when(mine > 0)
    def _():
        own_work()


    def wait_near(side):
        for count in range(1, PEERS + 1):
            @pl.when(near_count(side, count))
            def _():
                near_rows(side, count).wait_recv()

    split = (close - cells) // 2 + cells
    split = -(-split // 256) * 256

    def land_near(start, stop):
        source[:, start:stop] = near_buf[start - cells : stop - cells, :].astype(F32).T.astype(BF)

    wait_near(1)
    land_near(split, close)
    gather([split // 256], (close - split) // 256, True)

    wait_near(0)
    for side in (0, 1):
        @pl.when(inside(-1 if side else 1))
        def _():
            halo_copy(side).wait_recv()

    land_near(cells, split)
    side_slips = jnp.concatenate(
        [halo[...], jnp.zeros((LANES - 2 * HALO, LANES), BF)], axis=0
    ).astype(F32).T.astype(BF)
    stress = jnp.zeros(out_ref.shape, F32)
    for k in range(kinds):
        beside = near_cols[k * LANES : (k + 1) * LANES, :] + mm(
            side_slips, one_hot(LANES, near_rel[1, k : k + 1, :])
        ).astype(BF)
        stress = stress + mm(nb_ref[k], beside)
    out_ref[...] = stress
    gather([cells // 256], (split - cells) // 256, True)

    tops = [0]
    for bit in range(tree_bits):
        tops.append(tops[-1] + max(n >> bit, 32))
    top_spot = local_spots[-1]

    def whole_tree():
        place(0, roots[:, 0, :])
        for _ in rise(tops, [n >> bit for bit in range(tree_bits)], tree_bits - 1):
            yield
        spread(0, tops[-1], top_spot)
        yield

        def chosen(bit):
            both = terms[pl.ds(top_spot + tops[bit] // 2 + (me >> (bit + 1)), 1), :]
            both = jnp.broadcast_to(both, (8, 2 * LANES))
            return jnp.where((me >> bit) & 1 == 0, both[:, :LANES], both[:, LANES:])

        def half(both, bit):
            return jnp.where((me >> bit) & 1 == 0, both[:, :LANES], both[:, LANES:])

        line = lax.broadcasted_iota(jnp.int32, (8, LANES), 0)
        expansion = chosen(tree_bits - 1)
        bit = tree_bits - 2
        if tree_bits % 2 == 0 and bit >= 0:
            expansion = half(descend(expansion), bit) + chosen(bit)
            bit -= 1
            yield
        uppers = range(bit, 0, -2)
        aside = jnp.zeros((8, LANES), F32)
        for i, k in enumerate(uppers):
            aside = jnp.where(line == i, chosen(k), aside)
        aside = descend(aside)
        for i, k in enumerate(uppers):
            quarter = descend2(expansion)
            pair_half = jnp.where((me >> k) & 1 == 0, quarter[:, : 2 * LANES], quarter[:, 2 * LANES :])
            pair_half = pair_half + jnp.broadcast_to(aside[i : i + 1, :], pair_half.shape)
            expansion = half(pair_half, k - 1) + chosen(k - 1)
            yield
        rows = 1
        if local_levels % 2:
            both = descend(expansion)
            for c in range(2):
                loc[pl.ds(c, 8, stride=2), :] = both[:, c * LANES : (c + 1) * LANES]
            rows = 2
            expansion = loc[:8, :]
            yield
        while rows < cells:
            m = max(rows, 8)
            four = descend2(expansion)
            for c in range(4):
                loc[pl.ds(c, m, stride=4), :] = four[:, c * LANES : (c + 1) * LANES]
            rows *= 4
            expansion = loc[: max(rows, 8), :]
            yield

    root_rows().wait_recv()
    weave(
        whole_tree(),
        tree_bits + local_levels // 2,
        columns_of([wait_team(mine, True)], 1, True),
    )

    def finish(low, following):
        works = columns_of([low], 1, True)
        cut = types // 2
        for work in works[:cut]:
            work()
        low = None if following is None else wait_team(following, False)
        for work in works[cut:]:
            work()
        return low

    if teams <= 4:
        low = wait_team(mine ^ 1, False)
        for i in range(2, teams - 1):
            low = finish(low, mine ^ i)
        finish(low, None)
        finish(wait_team(mine ^ (teams - 1), False), None)
    else:
        def middle(i, carry):
            gather([wait_team(mine ^ i, False)], 1, True)
            return carry

        lax.fori_loop(1, teams, middle, 0)

    leaf_sum = mm(leaf_cat[...], columns[...])
    local_exp = ((loc[...] + own_loc[...]).T + leaf_sum)[:coef].astype(BF)
    out_ref[...] = out_ref[...] + mm(ts_ref[...], local_exp)

    far_rows(0, (n - 1) * CAP_FAR, 0).wait_send()
    root_rows().wait_send()
    for side in (0, 1):
        for count in range(1, PEERS + 1):
            @pl.when(near_count(side, count))
            def _():
                near_rows(side, count).wait_send()

    for side in (0, 1):
        @pl.when(inside(1 if side else -1))
        def _():
            halo_copy(side).wait_send()


def round_up(value, unit):
    return -(-value // unit) * unit


def body(*args):
    args = list(args)
    n = lax.axis_size("leaf")
    cells = args[0].shape[1]
    cap = args[8].shape[1] // n
    for i in (2, 3, 4):
        args[i] = jnp.transpose(args[i], (1, 0, 2))
    args[8] = jnp.reshape(args[8], (n, cap))
    slip, far_list, near_list = args[0], args[9], args[10]
    rest = cap - CAP_FAR
    peers = len(OFFSETS)
    total = cells + n * CAP_FAR + peers * rest
    dma = pltpu.SemaphoreType.DMA
    return pl.pallas_call(
        functools.partial(kernel, n, cells, cap),
        out_shape=pltpu.VMEM(slip.shape, F32),
        in_specs=[pl.BlockSpec(memory_space=pl.ANY)] * len(args),
        out_specs=pl.BlockSpec(memory_space=pltpu.VMEM),
        scratch_shapes=[pltpu.VMEM(a.shape, a.dtype) for a in args] + [
            pltpu.VMEM((n * CAP_FAR, LANES), BF),
            pltpu.VMEM((peers * cap, LANES), BF),
            pltpu.VMEM((n * CAP_FAR, LANES), BF),
            pltpu.VMEM((peers * rest, LANES), BF),
            pltpu.VMEM((2, HALO, LANES), BF),
            pltpu.VMEM((2 * HALO, LANES), BF),
            pltpu.VMEM((1, LANES), F32),
            pltpu.VMEM((n, 1, LANES), F32),
            pltpu.VMEM((n, cap), F32),
            pltpu.VMEM((n * CAP_FAR // LANES, LANES), F32),
            pltpu.VMEM((6, LANES, LANES), F32),
            pltpu.VMEM((2 * LANES, 2 * LANES), BF),
            pltpu.VMEM((2, 2 * LANES, 2 * LANES), BF),
            pltpu.VMEM((2 * LANES, 2 * LANES), BF),
            pltpu.VMEM((4 * LANES, 2 * LANES), BF),
            pltpu.VMEM((2 * LANES, 4 * LANES), BF),
            pltpu.VMEM((2 * cells + 2 * n + 512, LANES), F32),
            pltpu.VMEM((cells + n + 512, 2 * LANES), F32),
            pltpu.VMEM((cells, LANES), F32),
            pltpu.VMEM((cells, LANES), F32),
            pltpu.VMEM((total // 256, round_up(far_list.shape[0], 8), cells), F32),
            pltpu.VMEM((2, round_up(near_list.shape[0], 8), cells), F32),
            pltpu.VMEM((LANES, total), BF),
            pltpu.VMEM((LANES, far_list.shape[0] * LANES), BF),
            pltpu.VMEM((far_list.shape[0] * LANES, cells), BF),
            pltpu.VMEM((near_list.shape[0] * LANES, cells), BF),
            dma((len(args),)),
            pltpu.SemaphoreType.REGULAR((n * CAP_FAR // 256,)),
            dma,
            dma((n * CAP_FAR // 256,)),
            dma((2,)),
            dma((2,)),
            dma((2,)),
            dma((2,)),
            dma,
            dma,
        ],
        compiler_params=pltpu.CompilerParams(collective_id=0, has_side_effects=True),
    )(*args)


def solution(mesh):
    return jax.shard_map(
        body,
        mesh=mesh,
        in_specs=(
            P(None, "leaf"),
            P(),
            P(),
            P(),
            P(),
            P(),
            P(),
            P(),
            P("leaf", None),
            P(None, "leaf"),
            P(None, "leaf"),
        ),
        out_specs=P(None, "leaf"),
        check_vma=False,
    )
```

```python
import functools

import jax
import jax.numpy as jnp
from jax import lax
from jax.experimental import pallas as pl
from jax.experimental.pallas import tpu as pltpu
from jax.sharding import PartitionSpec as P

HALO = 32
PEERS = 4
CAP_FAR = 32
LANES = 128
BF = jnp.bfloat16
F32 = jnp.float32
MESH = pl.DeviceIdType.MESH
OFFSETS = tuple(range(-PEERS, 0)) + tuple(range(1, PEERS + 1))


def mm(a, b):
    return jnp.dot(a, b, preferred_element_type=F32)


def halves(x):
    high = x.astype(BF)
    return high, (x - high.astype(F32)).astype(BF)


def one_hot(rows, index):
    count = index.shape[1]
    lines = lax.broadcasted_iota(jnp.int32, (rows, count), 0).astype(F32).astype(BF)
    hit = lines == jnp.broadcast_to(index.astype(BF), (rows, count))
    return jnp.where(hit, jnp.ones((), BF), jnp.zeros((), BF))


def kernel(
    n, cells, cap,
    slip_any, tm_any, up_any, down_any, sib_any, leaf_any, ts_any, nb_any, send_any, far_any, near_any,
    out_ref,
    slip_ref, tm_ref, up_ref, down_ref, sib_ref, leaf_ref, ts_ref, nb_ref, send_ref, far_ref, near_ref,
    far_out, near_out, far_buf, near_buf, edges, halo, root_out, roots, send_f, far_idx,
    weight, w_up, w_sib, w_down, w_up2, w_down2, agg, terms, loc, own_loc, expansion_sum, rel, near_rel, source, leaf_cat, columns, near_cols, load_sem,
    above, far_send, far_recv, near_send, near_recv, halo_send, halo_recv, root_send, root_recv,
):
    me = lax.axis_index("leaf")
    coef = tm_ref.shape[0]
    types = far_ref.shape[0]
    kinds = near_ref.shape[0]
    rest = cap - CAP_FAR
    team = 256 // CAP_FAR
    teams = n // team
    mine = me // team
    close = cells + near_buf.shape[0]

    pairs = (
        (slip_any, slip_ref), (tm_any, tm_ref), (send_any, send_ref), (up_any, up_ref), (sib_any, sib_ref),
        (far_any, far_ref), (near_any, near_ref), (down_any, down_ref), (leaf_any, leaf_ref), (nb_any, nb_ref),
        (ts_any, ts_ref),
    )
    loads = [pltpu.make_async_copy(a, b, load_sem.at[i]) for i, (a, b) in enumerate(pairs)]
    for copy in loads:
        copy.start()

    barrier = pltpu.get_barrier_semaphore()

    far_buf[...] = jnp.zeros_like(far_buf)
    near_buf[...] = jnp.zeros_like(near_buf)
    halo[...] = jnp.zeros_like(halo)

    def greet(q, carry):
        pl.semaphore_signal(barrier, inc=1, device_id=(q,), device_id_type=MESH)
        return carry

    lax.fori_loop(me + 1, n, greet, 0)
    def answer(q, carry):
        pl.semaphore_signal(above.at[mine], inc=1, device_id=(q,), device_id_type=MESH)
        return carry

    weight[...] = jnp.zeros_like(weight)
    w_sib[...] = jnp.zeros_like(w_sib)
    leaf_cat[...] = jnp.zeros_like(leaf_cat)
    for copy in loads[:3]:
        copy.wait()

    weight[0, :coef, :] = tm_ref[...].astype(F32)
    multipole = mm(weight[0].astype(BF), slip_ref[...]).astype(BF)
    source[:, :cells] = multipole
    edges[0] = slip_ref[:, :LANES].astype(F32).T[:HALO].astype(BF)
    edges[1] = slip_ref[:, cells - LANES :].astype(F32).T[LANES - HALO :].astype(BF)

    def far_copy(target):
        return pltpu.make_async_remote_copy(
            src_ref=far_out.at[pl.ds(pl.multiple_of(target * CAP_FAR, CAP_FAR), CAP_FAR)],
            dst_ref=far_buf.at[pl.ds(pl.multiple_of(me * CAP_FAR, CAP_FAR), CAP_FAR)],
            send_sem=far_send,
            recv_sem=far_recv.at[mine],
            device_id=(target,),
            device_id_type=MESH,
        )

    def far_rows(start, rows, team_index):
        return pltpu.make_async_remote_copy(
            src_ref=far_out.at[pl.ds(start, rows)],
            dst_ref=far_buf.at[pl.ds(start, rows)],
            send_sem=far_send,
            recv_sem=far_recv.at[team_index],
            device_id=(lax.rem(me + 1, n),),
            device_id_type=MESH,
        )

    def near_copy(j):
        target = jnp.clip(me + OFFSETS[j], 0, n - 1)
        back = len(OFFSETS) - 1 - j
        return pltpu.make_async_remote_copy(
            src_ref=near_out.at[pl.ds(j * cap + CAP_FAR, rest)],
            dst_ref=near_buf.at[pl.ds(back * rest, rest)],
            send_sem=near_send.at[j // PEERS],
            recv_sem=near_recv.at[back // PEERS],
            device_id=(target,),
            device_id_type=MESH,
        )

    def near_rows(side, count):
        return pltpu.make_async_remote_copy(
            src_ref=near_out.at[pl.ds(0, count * rest)],
            dst_ref=near_buf.at[pl.ds(side * PEERS * rest, count * rest)],
            send_sem=near_send.at[side],
            recv_sem=near_recv.at[side],
            device_id=(lax.rem(me + 1, n),),
            device_id_type=MESH,
        )

    def near_count(side, count):
        reach = n - 1 - me if side else me
        return reach >= count if count == PEERS else reach == count

    def halo_copy(side):
        target = jnp.clip(me + (1 if side else -1), 0, n - 1)
        return pltpu.make_async_remote_copy(
            src_ref=edges.at[side],
            dst_ref=halo.at[pl.ds((1 - side) * HALO, HALO)],
            send_sem=halo_send.at[side],
            recv_sem=halo_recv.at[1 - side],
            device_id=(target,),
            device_id_type=MESH,
        )

    def root_copy(target):
        return pltpu.make_async_remote_copy(
            src_ref=root_out,
            dst_ref=roots.at[me],
            send_sem=root_send,
            recv_sem=root_recv,
            device_id=(target,),
            device_id_type=MESH,
        )

    def root_rows():
        return pltpu.make_async_remote_copy(
            src_ref=roots.at[pl.ds(0, n - 1)],
            dst_ref=roots.at[pl.ds(0, n - 1)],
            send_sem=root_send,
            recv_sem=root_recv,
            device_id=(lax.rem(me + 1, n),),
            device_id_type=MESH,
        )

    def inside(offset):
        return jnp.logical_and(me + offset >= 0, me + offset < n)

    send_f[...] = send_ref[...].astype(F32)
    per_row = LANES // CAP_FAR
    strip = 8 * per_row
    lane = lax.broadcasted_iota(jnp.int32, (8, LANES), 1)
    for g in range(n // strip):
        packed = send_f[pl.ds(g * strip, 8, stride=per_row), :]
        for j in range(1, per_row):
            shifted = pltpu.roll(send_f[pl.ds(g * strip + j, 8, stride=per_row), :], j * CAP_FAR, axis=1)
            packed = jnp.where(lane >= j * CAP_FAR, shifted, packed)
        far_idx[g * 8 : (g + 1) * 8, :] = packed

    def pick(first, second):
        hits = jnp.concatenate([one_hot(cells, first), one_hot(cells, second)], axis=1)
        return mm(multipole, hits).T.astype(BF)

    def pick_far(g):
        far_out[g * 256 : (g + 1) * 256, :] = pick(far_idx[2 * g : 2 * g + 1, :], far_idx[2 * g + 1 : 2 * g + 2, :])

    def pick_near(j):
        first, second = (
            send_f[pl.ds(jnp.clip(me + OFFSETS[i], 0, n - 1), 1), :] for i in (j, j + 1)
        )
        near_out[j * cap : (j + 2) * cap, :] = pick(first, second)

    for j in range(0, len(OFFSETS), 2):
        pick_near(j)

    def weave(chain, count, fillers):
        done = 0
        for i, _ in enumerate(chain):
            upto = min(len(fillers), -(-len(fillers) * (i + 1) // count))
            for work in fillers[done:upto]:
                work()
            done = upto
        for work in fillers[done:]:
            work()

    def send_far(low, high, lower):
        def step(i, carry):
            group = i // team if lower else jnp.where(mine == 0, lax.rem(i // team, teams), mine + teams - i // team)
            target = group * team + lax.rem(me + i, team)

            @pl.when(target < me if lower else target > me)
            def _():
                far_copy(target).start()

            return carry

        lax.fori_loop(low, high, step, 0)

    def send_near(wanted):
        for j, offset in enumerate(OFFSETS):
            if (offset < 0) == (wanted is None):
                place_of = me + offset
                ready = place_of >= 0 if wanted is None else jnp.logical_and(place_of < n, place_of // team == wanted)

                @pl.when(ready)
                def _():
                    near_copy(j).start()

    def send_root(low, high):
        def step(q, carry):
            root_copy(q).start()
            return carry

        lax.fori_loop(low, high, step, 0)

    def first_sends():
        @pl.when(me > 0)
        def _():
            pl.semaphore_wait(barrier, me)
            halo_copy(0).start()

        lax.fori_loop(0, me, answer, 0)
        send_near(None)

    late = lax.rem(me, team) < 2

    @pl.when(jnp.logical_not(late))
    def _():
        first_sends()

    for copy in loads[3:8]:
        copy.wait()

    def parts(ref, index):
        weight[index, :coef, :coef] = ref
        weight[index, :coef, coef:] = jnp.zeros((coef, LANES - coef), F32)
        return halves(weight[index].T)

    def product(highs, lows):
        tall = [jnp.concatenate(x, axis=0) for x in (highs, lows)]
        wide = [jnp.concatenate(x, axis=1) for x in (highs, lows)]
        return halves(mm(tall[0], wide[0]) + mm(tall[0], wide[1]) + mm(tall[1], wide[0]))

    ups = [parts(up_ref[:, s, :], s) for s in (0, 1)]
    for s in (0, 1):
        w_up[s * LANES : (s + 1) * LANES, :LANES] = ups[s][0]
        w_up[s * LANES : (s + 1) * LANES, LANES:] = ups[s][1]
    for i, both in enumerate(product(*zip(*ups))):
        for c in range(4):
            w_up2[c * LANES : (c + 1) * LANES, i * LANES : (i + 1) * LANES] = both[
                (c & 1) * LANES : ((c & 1) + 1) * LANES, (c >> 1) * LANES : ((c >> 1) + 1) * LANES
            ]

    def prepare():
        for s in (0, 1):
            high, low = parts(sib_ref[:, s, :], 4 + s)
            other = 1 - s
            w_sib[0, other * LANES : (other + 1) * LANES, s * LANES : (s + 1) * LANES] = high
            w_sib[1, other * LANES : (other + 1) * LANES, s * LANES : (s + 1) * LANES] = low
        downs = [parts(down_ref[:, s, :], 2 + s) for s in (0, 1)]
        for s in (0, 1):
            w_down[:LANES, s * LANES : (s + 1) * LANES] = downs[s][0]
            w_down[LANES:, s * LANES : (s + 1) * LANES] = downs[s][1]
        for i, both in enumerate(product(*zip(*downs))):
            for s in (0, 1):
                w_down2[i * LANES : (i + 1) * LANES, 2 * s * LANES : 2 * (s + 1) * LANES] = both[
                    s * LANES : (s + 1) * LANES, :
                ]

    def pair(base, rows):
        m = max(rows // 2, 8)
        even = agg[pl.ds(base, m, stride=2), :]
        odd = agg[pl.ds(base + 1, m, stride=2), :]
        return m, halves(jnp.concatenate([even, odd], axis=1))

    def lift(base, rows):
        _, (high, low) = pair(base, rows)
        first = mm(high, w_up[...])
        second = mm(low, w_up[:, :LANES])
        return first[:, :LANES] + first[:, LANES:] + second

    def lift2(base, rows):
        m = max(rows // 4, 8)
        four = [agg[pl.ds(base + c, m, stride=4), :] for c in range(4)]
        high, low = halves(jnp.concatenate(four, axis=1))
        first = mm(high, w_up2[...])
        second = mm(low, w_up2[:, :LANES])
        return first[:, :LANES] + first[:, LANES:] + second

    def across(high, low):
        return mm(high, w_sib[0]) + mm(high, w_sib[1]) + mm(low, w_sib[0])

    def place(base, value):
        agg[base : base + value.shape[0], :] = value
        if value.shape[0] < 32:
            agg[base + value.shape[0] : base + 32, :] = jnp.zeros((32 - value.shape[0], LANES), F32)

    local_levels = cells.bit_length() - 1
    tree_bits = n.bit_length() - 1
    agg[:cells, :] = multipole.astype(F32).T
    bases = [0]
    for height in range(local_levels):
        bases.append(bases[-1] + max(cells >> height, 32))
    local_spots = [(base - cells) // 2 for base in bases]

    def spread(start, stop, spot):
        m = (stop - start) // 2
        even = agg[pl.ds(start, m, stride=2), :]
        odd = agg[pl.ds(start + 1, m, stride=2), :]
        terms[spot : spot + m, :] = across(*halves(jnp.concatenate([even, odd], axis=1)))

    def rise(bases, sizes, last):
        for height in range(0, last, 2):
            value = None
            if height + 2 <= last:
                value = lift2(bases[height], sizes[height])
                place(bases[height + 2], value)
            if height + 1 <= last:
                below = lift(bases[height], sizes[height])
                place(bases[height + 1], below)
                value = below if value is None else value
            yield value

    def climb():
        for value in rise(bases, [cells >> h for h in range(local_levels + 1)], local_levels):
            yield
        root_out[...] = value[:1]
        roots[me] = value[:1]

    def beside_own(k):
        near_cols[k * LANES : (k + 1) * LANES, :] = mm(
            slips, one_hot(cells, near_rel[0, k : k + 1, :])
        ).astype(BF)

    def column(t, starts, count, more):
        found = sum(
            mm(
                source[:, pl.ds(pl.multiple_of(low * 256, 256), count * 256)],
                jnp.concatenate([one_hot(256, rel[low + b, t : t + 1, :]) for b in range(count)], axis=0),
            )
            for low in starts
        ).astype(BF)
        if more:
            found = found + columns[t * LANES : (t + 1) * LANES, :]
        columns[t * LANES : (t + 1) * LANES, :] = found

    def columns_of(starts, count, more):
        return [functools.partial(column, t, starts, count, more) for t in range(types)]

    def gather(starts, count, more):
        for work in columns_of(starts, count, more):
            work()

    weave(
        climb(),
        (local_levels + 1) // 2,
        [functools.partial(pick_far, g) for g in range(n // (2 * per_row))],
    )

    @pl.when(late)
    def _():
        first_sends()

    send_root(0, me)

    @pl.when(mine > 0)
    def _():
        send_far(0, team, True)

    @pl.when(lax.rem(me, team) < team - 1)
    def _():
        pl.semaphore_wait(above.at[mine], team - 1 - lax.rem(me, team))
        halo_copy(1).start()

    send_root(me + 1, (mine + 1) * team)
    send_near(mine)

    @pl.when(mine + 1 < teams)
    def _():
        pl.semaphore_wait(above.at[mine + 1], team)

        @pl.when(lax.rem(me, team) == team - 1)
        def _():
            halo_copy(1).start()

        send_near(mine + 1)
        send_root((mine + 1) * team, (mine + 2) * team)

    send_far(jnp.minimum(mine, 1) * team, (mine + 1) * team, True)
    send_far(n, n + team, False)

    for copy in loads[8:]:
        copy.wait()

    v = far_ref[...]
    behind = v - cells
    sender = behind // cap
    slot = behind % cap
    delta = sender - me
    hop = jnp.where(delta < 0, delta + PEERS, delta + PEERS - 1)
    position = jnp.where(
        v < cells,
        v,
        jnp.where(
            slot < CAP_FAR,
            close + sender * CAP_FAR + slot,
            cells + hop * rest + slot - CAP_FAR,
        ),
    )
    total = source.shape[1]
    blocks = total // 256
    for b in range(blocks):
        rel[b, :types, :] = jnp.clip(position - 256 * b, -1, 256).astype(F32)

    w = near_ref[...]
    near_rel[0, :kinds, :] = jnp.clip(w - HALO, -1, cells).astype(F32)
    near_rel[1, :kinds, :] = jnp.where(
        w < HALO, w, jnp.where(w >= HALO + cells, w - cells, -1)
    ).astype(F32)
    slips = slip_ref[...]

    def wait_team(index, own):
        start = pl.multiple_of(index * 256, 256)
        if own:
            far_rows(start, 256 - CAP_FAR, index).wait_recv()
        else:
            far_rows(start, 256, index).wait_recv()
        source[:, pl.ds(close + start, 256)] = far_buf[pl.ds(start, 256), :].astype(F32).T.astype(BF)
        return close // 256 + index

    prepare()

    def descend(x):
        high, low = halves(x)
        return mm(high, w_down[:LANES, :]) + mm(high, w_down[LANES:, :]) + mm(low, w_down[:LANES, :])

    def descend2(x):
        high, low = halves(x)
        return mm(high, w_down2[:LANES, :]) + mm(high, w_down2[LANES:, :]) + mm(low, w_down2[:LANES, :])

    def settle():
        spread(bases[1], bases[-1], 0)
        yield
        expansion = None
        for height in reversed(range(local_levels)):
            m = max((cells >> height) // 2, 8)
            both = None if expansion is None else descend(expansion)
            if height >= 1:
                term = terms[local_spots[height] : local_spots[height] + m, :]
                both = term if both is None else both + term
            own_loc[pl.ds(0, m, stride=2), :] = both[:, :LANES]
            own_loc[pl.ds(1, m, stride=2), :] = both[:, LANES:]
            expansion = own_loc[: max(cells >> height, 8), :]
            yield

    def lay(t):
        leaf_cat[:coef, t * LANES : t * LANES + coef] = leaf_ref[t]

    def own_work():
        weave(
            settle(),
            local_levels + 1,
            columns_of([0], cells // 256, False)
            + [functools.partial(beside_own, k) for k in range(kinds)]
            + [functools.partial(lay, t) for t in range(types)],
        )

    @pl.when(mine == 0)
    def _():
        own_work()

    def send_rest(index, carry):
        pl.semaphore_wait(above.at[index], team)
        send_root(index * team, (index + 1) * team)
        return carry

    lax.fori_loop(mine + 2, teams, send_rest, 0)
    send_far((mine + 1) * team, n, False)

    @pl.when(mine > 0)
    def _():
        own_work()


    def wait_near(side):
        for count in range(1, PEERS + 1):
            @pl.when(near_count(side, count))
            def _():
                near_rows(side, count).wait_recv()

    split = (close - cells) // 2 + cells
    split = -(-split // 256) * 256

    def land_near(start, stop):
        source[:, start:stop] = near_buf[start - cells : stop - cells, :].astype(F32).T.astype(BF)

    wait_near(1)
    land_near(split, close)
    gather([split // 256], (close - split) // 256, True)

    wait_near(0)
    for side in (0, 1):
        @pl.when(inside(-1 if side else 1))
        def _():
            halo_copy(side).wait_recv()

    land_near(cells, split)
    side_slips = jnp.concatenate(
        [halo[...], jnp.zeros((LANES - 2 * HALO, LANES), BF)], axis=0
    ).astype(F32).T.astype(BF)
    stress = jnp.zeros(out_ref.shape, F32)
    for k in range(kinds):
        beside = near_cols[k * LANES : (k + 1) * LANES, :] + mm(
            side_slips, one_hot(LANES, near_rel[1, k : k + 1, :])
        ).astype(BF)
        stress = stress + mm(nb_ref[k], beside)
    out_ref[...] = stress
    gather([cells // 256], (split - cells) // 256, True)

    tops = [0]
    for bit in range(tree_bits):
        tops.append(tops[-1] + max(n >> bit, 32))
    top_spot = local_spots[-1]

    def whole_tree():
        place(0, roots[:, 0, :])
        for _ in rise(tops, [n >> bit for bit in range(tree_bits)], tree_bits - 1):
            yield
        spread(0, tops[-1], top_spot)
        yield

        def chosen(bit):
            both = terms[pl.ds(top_spot + tops[bit] // 2 + (me >> (bit + 1)), 1), :]
            both = jnp.broadcast_to(both, (8, 2 * LANES))
            return jnp.where((me >> bit) & 1 == 0, both[:, :LANES], both[:, LANES:])

        def half(both, bit):
            return jnp.where((me >> bit) & 1 == 0, both[:, :LANES], both[:, LANES:])

        line = lax.broadcasted_iota(jnp.int32, (8, LANES), 0)
        expansion = chosen(tree_bits - 1)
        bit = tree_bits - 2
        if tree_bits % 2 == 0 and bit >= 0:
            expansion = half(descend(expansion), bit) + chosen(bit)
            bit -= 1
            yield
        uppers = range(bit, 0, -2)
        aside = jnp.zeros((8, LANES), F32)
        for i, k in enumerate(uppers):
            aside = jnp.where(line == i, chosen(k), aside)
        aside = descend(aside)
        for i, k in enumerate(uppers):
            quarter = descend2(expansion)
            pair_half = jnp.where((me >> k) & 1 == 0, quarter[:, : 2 * LANES], quarter[:, 2 * LANES :])
            pair_half = pair_half + jnp.broadcast_to(aside[i : i + 1, :], pair_half.shape)
            expansion = half(pair_half, k - 1) + chosen(k - 1)
            yield
        rows = 1
        if local_levels % 2:
            both = descend(expansion)
            for c in range(2):
                loc[pl.ds(c, 8, stride=2), :] = both[:, c * LANES : (c + 1) * LANES]
            rows = 2
            expansion = loc[:8, :]
            yield
        while rows < cells:
            m = max(rows, 8)
            four = descend2(expansion)
            for c in range(4):
                loc[pl.ds(c, m, stride=4), :] = four[:, c * LANES : (c + 1) * LANES]
            rows *= 4
            expansion = loc[: max(rows, 8), :]
            yield

    root_rows().wait_recv()
    weave(
        whole_tree(),
        tree_bits + local_levels // 2,
        columns_of([wait_team(mine, True)], 1, True),
    )

    if teams <= 4:
        gather([wait_team(mine ^ i, False) for i in range(1, teams - 1)], 1, True)
        last = wait_team(mine ^ (teams - 1), False)
    else:
        def middle(i, carry):
            gather([wait_team(mine ^ i, False)], 1, True)
            return carry

        lax.fori_loop(1, teams - 1, middle, 0)
        last = wait_team(mine ^ (teams - 1), False)

    expansion_sum[...] = (loc[...] + own_loc[...]).T
    works = columns_of([last], 1, True)
    parts_of = 2
    marks = [types * i // parts_of for i in range(parts_of + 1)]
    for first, stop in zip(marks[:-1], marks[1:]):
        for work in works[first:stop]:
            work()
        span = slice(first * LANES, stop * LANES)
        found = expansion_sum[...] + mm(leaf_cat[:, span], columns[span, :])
        if stop < types:
            expansion_sum[...] = found
    local_exp = found[:coef].astype(BF)
    out_ref[...] = out_ref[...] + mm(ts_ref[...], local_exp)

    far_rows(0, (n - 1) * CAP_FAR, 0).wait_send()
    root_rows().wait_send()
    for side in (0, 1):
        for count in range(1, PEERS + 1):
            @pl.when(near_count(side, count))
            def _():
                near_rows(side, count).wait_send()

    for side in (0, 1):
        @pl.when(inside(1 if side else -1))
        def _():
            halo_copy(side).wait_send()


def round_up(value, unit):
    return -(-value // unit) * unit


def body(*args):
    args = list(args)
    n = lax.axis_size("leaf")
    cells = args[0].shape[1]
    cap = args[8].shape[1] // n
    for i in (2, 3, 4):
        args[i] = jnp.transpose(args[i], (1, 0, 2))
    args[8] = jnp.reshape(args[8], (n, cap))
    slip, far_list, near_list = args[0], args[9], args[10]
    rest = cap - CAP_FAR
    peers = len(OFFSETS)
    total = cells + n * CAP_FAR + peers * rest
    dma = pltpu.SemaphoreType.DMA
    return pl.pallas_call(
        functools.partial(kernel, n, cells, cap),
        out_shape=pltpu.VMEM(slip.shape, F32),
        in_specs=[pl.BlockSpec(memory_space=pl.ANY)] * len(args),
        out_specs=pl.BlockSpec(memory_space=pltpu.VMEM),
        scratch_shapes=[pltpu.VMEM(a.shape, a.dtype) for a in args] + [
            pltpu.VMEM((n * CAP_FAR, LANES), BF),
            pltpu.VMEM((peers * cap, LANES), BF),
            pltpu.VMEM((n * CAP_FAR, LANES), BF),
            pltpu.VMEM((peers * rest, LANES), BF),
            pltpu.VMEM((2, HALO, LANES), BF),
            pltpu.VMEM((2 * HALO, LANES), BF),
            pltpu.VMEM((1, LANES), F32),
            pltpu.VMEM((n, 1, LANES), F32),
            pltpu.VMEM((n, cap), F32),
            pltpu.VMEM((n * CAP_FAR // LANES, LANES), F32),
            pltpu.VMEM((6, LANES, LANES), F32),
            pltpu.VMEM((2 * LANES, 2 * LANES), BF),
            pltpu.VMEM((2, 2 * LANES, 2 * LANES), BF),
            pltpu.VMEM((2 * LANES, 2 * LANES), BF),
            pltpu.VMEM((4 * LANES, 2 * LANES), BF),
            pltpu.VMEM((2 * LANES, 4 * LANES), BF),
            pltpu.VMEM((2 * cells + 2 * n + 512, LANES), F32),
            pltpu.VMEM((cells + n + 512, 2 * LANES), F32),
            pltpu.VMEM((cells, LANES), F32),
            pltpu.VMEM((cells, LANES), F32),
            pltpu.VMEM((LANES, cells), F32),
            pltpu.VMEM((total // 256, round_up(far_list.shape[0], 8), cells), F32),
            pltpu.VMEM((2, round_up(near_list.shape[0], 8), cells), F32),
            pltpu.VMEM((LANES, total), BF),
            pltpu.VMEM((LANES, far_list.shape[0] * LANES), BF),
            pltpu.VMEM((far_list.shape[0] * LANES, cells), BF),
            pltpu.VMEM((near_list.shape[0] * LANES, cells), BF),
            dma((len(args),)),
            pltpu.SemaphoreType.REGULAR((n * CAP_FAR // 256,)),
            dma,
            dma((n * CAP_FAR // 256,)),
            dma((2,)),
            dma((2,)),
            dma((2,)),
            dma((2,)),
            dma,
            dma,
        ],
        compiler_params=pltpu.CompilerParams(collective_id=0, has_side_effects=True),
    )(*args)


def solution(mesh):
    return jax.shard_map(
        body,
        mesh=mesh,
        in_specs=(
            P(None, "leaf"),
            P(),
            P(),
            P(),
            P(),
            P(),
            P(),
            P(),
            P("leaf", None),
            P(None, "leaf"),
            P(None, "leaf"),
        ),
        out_specs=P(None, "leaf"),
        check_vma=False,
    )
```

```python
import functools

import jax
import jax.numpy as jnp
from jax import lax
from jax.experimental import pallas as pl
from jax.experimental.pallas import tpu as pltpu
from jax.sharding import PartitionSpec as P

HALO = 32
PEERS = 4
CAP_FAR = 32
LANES = 128
BF = jnp.bfloat16
F32 = jnp.float32
MESH = pl.DeviceIdType.MESH
OFFSETS = tuple(range(-PEERS, 0)) + tuple(range(1, PEERS + 1))


def mm(a, b):
    return jnp.dot(a, b, preferred_element_type=F32)


def halves(x):
    high = x.astype(BF)
    return high, (x - high.astype(F32)).astype(BF)


def one_hot(rows, index):
    count = index.shape[1]
    lines = lax.broadcasted_iota(jnp.int32, (rows, count), 0).astype(F32).astype(BF)
    hit = lines == jnp.broadcast_to(index.astype(BF), (rows, count))
    return jnp.where(hit, jnp.ones((), BF), jnp.zeros((), BF))


def kernel(
    n, cells, cap,
    slip_any, tm_any, up_any, down_any, sib_any, leaf_any, ts_any, nb_any, send_any, far_any, near_any,
    out_ref,
    slip_ref, tm_ref, up_ref, down_ref, sib_ref, leaf_ref, ts_ref, nb_ref, send_ref, far_ref, near_ref,
    far_out, near_out, far_buf, near_buf, edges, halo, root_out, roots, send_f, far_idx,
    weight, w_up, w_sib, w_down, w_up2, w_down2, agg, terms, loc, own_loc, expansion_sum, rel, near_rel, source, leaf_cat, columns, near_cols, load_sem,
    above, far_send, far_recv, near_send, near_recv, halo_send, halo_recv, root_send, root_recv,
):
    me = lax.axis_index("leaf")
    coef = tm_ref.shape[0]
    types = far_ref.shape[0]
    kinds = near_ref.shape[0]
    rest = cap - CAP_FAR
    team = 256 // CAP_FAR
    teams = n // team
    mine = me // team
    close = cells + near_buf.shape[0]

    pairs = (
        (slip_any, slip_ref), (tm_any, tm_ref), (send_any, send_ref), (up_any, up_ref), (sib_any, sib_ref),
        (far_any, far_ref), (near_any, near_ref), (down_any, down_ref), (leaf_any, leaf_ref), (nb_any, nb_ref),
        (ts_any, ts_ref),
    )
    loads = [pltpu.make_async_copy(a, b, load_sem.at[i]) for i, (a, b) in enumerate(pairs)]
    for copy in loads:
        copy.start()

    barrier = pltpu.get_barrier_semaphore()

    far_buf[...] = jnp.zeros_like(far_buf)
    near_buf[...] = jnp.zeros_like(near_buf)
    halo[...] = jnp.zeros_like(halo)

    def greet(q, carry):
        pl.semaphore_signal(barrier, inc=1, device_id=(q,), device_id_type=MESH)
        return carry

    lax.fori_loop(me + 1, n, greet, 0)
    def answer(q, carry):
        pl.semaphore_signal(above.at[mine], inc=1, device_id=(q,), device_id_type=MESH)
        return carry

    weight[...] = jnp.zeros_like(weight)
    w_sib[...] = jnp.zeros_like(w_sib)
    leaf_cat[...] = jnp.zeros_like(leaf_cat)
    for copy in loads[:3]:
        copy.wait()

    weight[0, :coef, :] = tm_ref[...].astype(F32)
    multipole = mm(weight[0].astype(BF), slip_ref[...]).astype(BF)
    source[:, :cells] = multipole
    edges[0] = slip_ref[:, :LANES].astype(F32).T[:HALO].astype(BF)
    edges[1] = slip_ref[:, cells - LANES :].astype(F32).T[LANES - HALO :].astype(BF)

    def far_copy(target):
        return pltpu.make_async_remote_copy(
            src_ref=far_out.at[pl.ds(pl.multiple_of(target * CAP_FAR, CAP_FAR), CAP_FAR)],
            dst_ref=far_buf.at[pl.ds(pl.multiple_of(me * CAP_FAR, CAP_FAR), CAP_FAR)],
            send_sem=far_send,
            recv_sem=far_recv.at[mine],
            device_id=(target,),
            device_id_type=MESH,
        )

    def far_rows(start, rows, team_index):
        return pltpu.make_async_remote_copy(
            src_ref=far_out.at[pl.ds(start, rows)],
            dst_ref=far_buf.at[pl.ds(start, rows)],
            send_sem=far_send,
            recv_sem=far_recv.at[team_index],
            device_id=(lax.rem(me + 1, n),),
            device_id_type=MESH,
        )

    def near_copy(j):
        target = jnp.clip(me + OFFSETS[j], 0, n - 1)
        back = len(OFFSETS) - 1 - j
        return pltpu.make_async_remote_copy(
            src_ref=near_out.at[pl.ds(j * cap + CAP_FAR, rest)],
            dst_ref=near_buf.at[pl.ds(back * rest, rest)],
            send_sem=near_send.at[j // PEERS],
            recv_sem=near_recv.at[back // PEERS],
            device_id=(target,),
            device_id_type=MESH,
        )

    def near_rows(side, count):
        return pltpu.make_async_remote_copy(
            src_ref=near_out.at[pl.ds(0, count * rest)],
            dst_ref=near_buf.at[pl.ds(side * PEERS * rest, count * rest)],
            send_sem=near_send.at[side],
            recv_sem=near_recv.at[side],
            device_id=(lax.rem(me + 1, n),),
            device_id_type=MESH,
        )

    def near_count(side, count):
        reach = n - 1 - me if side else me
        return reach >= count if count == PEERS else reach == count

    def halo_copy(side):
        target = jnp.clip(me + (1 if side else -1), 0, n - 1)
        return pltpu.make_async_remote_copy(
            src_ref=edges.at[side],
            dst_ref=halo.at[pl.ds((1 - side) * HALO, HALO)],
            send_sem=halo_send.at[side],
            recv_sem=halo_recv.at[1 - side],
            device_id=(target,),
            device_id_type=MESH,
        )

    def root_copy(target):
        return pltpu.make_async_remote_copy(
            src_ref=root_out,
            dst_ref=roots.at[me],
            send_sem=root_send,
            recv_sem=root_recv,
            device_id=(target,),
            device_id_type=MESH,
        )

    def root_rows():
        return pltpu.make_async_remote_copy(
            src_ref=roots.at[pl.ds(0, n - 1)],
            dst_ref=roots.at[pl.ds(0, n - 1)],
            send_sem=root_send,
            recv_sem=root_recv,
            device_id=(lax.rem(me + 1, n),),
            device_id_type=MESH,
        )

    def inside(offset):
        return jnp.logical_and(me + offset >= 0, me + offset < n)

    send_f[...] = send_ref[...].astype(F32)
    per_row = LANES // CAP_FAR
    strip = 8 * per_row
    lane = lax.broadcasted_iota(jnp.int32, (8, LANES), 1)
    for g in range(n // strip):
        packed = send_f[pl.ds(g * strip, 8, stride=per_row), :]
        for j in range(1, per_row):
            shifted = pltpu.roll(send_f[pl.ds(g * strip + j, 8, stride=per_row), :], j * CAP_FAR, axis=1)
            packed = jnp.where(lane >= j * CAP_FAR, shifted, packed)
        far_idx[g * 8 : (g + 1) * 8, :] = packed

    def pick(first, second):
        hits = jnp.concatenate([one_hot(cells, first), one_hot(cells, second)], axis=1)
        return mm(multipole, hits).T.astype(BF)

    def pick_far(g):
        far_out[g * 256 : (g + 1) * 256, :] = pick(far_idx[2 * g : 2 * g + 1, :], far_idx[2 * g + 1 : 2 * g + 2, :])

    def pick_near(j):
        first, second = (
            send_f[pl.ds(jnp.clip(me + OFFSETS[i], 0, n - 1), 1), :] for i in (j, j + 1)
        )
        near_out[j * cap : (j + 2) * cap, :] = pick(first, second)

    for j in range(0, len(OFFSETS), 2):
        pick_near(j)

    def weave(chain, count, fillers):
        done = 0
        for i, _ in enumerate(chain):
            upto = min(len(fillers), -(-len(fillers) * (i + 1) // count))
            for work in fillers[done:upto]:
                work()
            done = upto
        for work in fillers[done:]:
            work()

    def send_far(low, high, lower):
        def step(i, carry):
            group = i // team if lower else jnp.where(mine == 0, lax.rem(i // team, teams), mine + teams - i // team)
            target = group * team + lax.rem(me + i, team)

            @pl.when(target < me if lower else target > me)
            def _():
                far_copy(target).start()

            return carry

        lax.fori_loop(low, high, step, 0)

    def send_near(wanted):
        for j, offset in enumerate(OFFSETS):
            if (offset < 0) == (wanted is None):
                place_of = me + offset
                ready = place_of >= 0 if wanted is None else jnp.logical_and(place_of < n, place_of // team == wanted)

                @pl.when(ready)
                def _():
                    near_copy(j).start()

    def send_root(low, high):
        def step(q, carry):
            root_copy(q).start()
            return carry

        lax.fori_loop(low, high, step, 0)

    def first_sends():
        @pl.when(me > 0)
        def _():
            pl.semaphore_wait(barrier, me)
            halo_copy(0).start()

        lax.fori_loop(0, me, answer, 0)
        send_near(None)

    late = lax.rem(me, team) < 2

    @pl.when(jnp.logical_not(late))
    def _():
        first_sends()

    for copy in loads[3:8]:
        copy.wait()

    def parts(ref, index):
        weight[index, :coef, :coef] = ref
        weight[index, :coef, coef:] = jnp.zeros((coef, LANES - coef), F32)
        return halves(weight[index].T)

    def product(highs, lows):
        tall = [jnp.concatenate(x, axis=0) for x in (highs, lows)]
        wide = [jnp.concatenate(x, axis=1) for x in (highs, lows)]
        return halves(mm(tall[0], wide[0]) + mm(tall[0], wide[1]) + mm(tall[1], wide[0]))

    ups = [parts(up_ref[:, s, :], s) for s in (0, 1)]
    for s in (0, 1):
        w_up[s * LANES : (s + 1) * LANES, :LANES] = ups[s][0]
        w_up[s * LANES : (s + 1) * LANES, LANES:] = ups[s][1]
    for i, both in enumerate(product(*zip(*ups))):
        for c in range(4):
            w_up2[c * LANES : (c + 1) * LANES, i * LANES : (i + 1) * LANES] = both[
                (c & 1) * LANES : ((c & 1) + 1) * LANES, (c >> 1) * LANES : ((c >> 1) + 1) * LANES
            ]

    def prepare():
        for s in (0, 1):
            high, low = parts(sib_ref[:, s, :], 4 + s)
            other = 1 - s
            w_sib[0, other * LANES : (other + 1) * LANES, s * LANES : (s + 1) * LANES] = high
            w_sib[1, other * LANES : (other + 1) * LANES, s * LANES : (s + 1) * LANES] = low
        downs = [parts(down_ref[:, s, :], 2 + s) for s in (0, 1)]
        for s in (0, 1):
            w_down[:LANES, s * LANES : (s + 1) * LANES] = downs[s][0]
            w_down[LANES:, s * LANES : (s + 1) * LANES] = downs[s][1]
        for i, both in enumerate(product(*zip(*downs))):
            for s in (0, 1):
                w_down2[i * LANES : (i + 1) * LANES, 2 * s * LANES : 2 * (s + 1) * LANES] = both[
                    s * LANES : (s + 1) * LANES, :
                ]

    def pair(base, rows):
        m = max(rows // 2, 8)
        even = agg[pl.ds(base, m, stride=2), :]
        odd = agg[pl.ds(base + 1, m, stride=2), :]
        return m, halves(jnp.concatenate([even, odd], axis=1))

    def lift(base, rows):
        _, (high, low) = pair(base, rows)
        first = mm(high, w_up[...])
        second = mm(low, w_up[:, :LANES])
        return first[:, :LANES] + first[:, LANES:] + second

    def lift2(base, rows):
        m = max(rows // 4, 8)
        four = [agg[pl.ds(base + c, m, stride=4), :] for c in range(4)]
        high, low = halves(jnp.concatenate(four, axis=1))
        first = mm(high, w_up2[...])
        second = mm(low, w_up2[:, :LANES])
        return first[:, :LANES] + first[:, LANES:] + second

    def across(high, low):
        return mm(high, w_sib[0]) + mm(high, w_sib[1]) + mm(low, w_sib[0])

    def place(base, value):
        agg[base : base + value.shape[0], :] = value
        if value.shape[0] < 32:
            agg[base + value.shape[0] : base + 32, :] = jnp.zeros((32 - value.shape[0], LANES), F32)

    local_levels = cells.bit_length() - 1
    tree_bits = n.bit_length() - 1
    agg[:cells, :] = multipole.astype(F32).T
    bases = [0]
    for height in range(local_levels):
        bases.append(bases[-1] + max(cells >> height, 32))
    local_spots = [(base - cells) // 2 for base in bases]

    def spread(start, stop, spot):
        m = (stop - start) // 2
        even = agg[pl.ds(start, m, stride=2), :]
        odd = agg[pl.ds(start + 1, m, stride=2), :]
        terms[spot : spot + m, :] = across(*halves(jnp.concatenate([even, odd], axis=1)))

    def rise(bases, sizes, last):
        for height in range(0, last, 2):
            value = None
            if height + 2 <= last:
                value = lift2(bases[height], sizes[height])
                place(bases[height + 2], value)
            if height + 1 <= last:
                below = lift(bases[height], sizes[height])
                place(bases[height + 1], below)
                value = below if value is None else value
            yield value

    def climb():
        for value in rise(bases, [cells >> h for h in range(local_levels + 1)], local_levels):
            yield
        root_out[...] = value[:1]
        roots[me] = value[:1]

    def beside_own(k):
        near_cols[k * LANES : (k + 1) * LANES, :] = mm(
            slips, one_hot(cells, near_rel[0, k : k + 1, :])
        ).astype(BF)

    def column(t, starts, count, more):
        found = sum(
            mm(
                source[:, pl.ds(pl.multiple_of(low * 256, 256), count * 256)],
                jnp.concatenate([one_hot(256, rel[low + b, t : t + 1, :]) for b in range(count)], axis=0),
            )
            for low in starts
        ).astype(BF)
        if more:
            found = found + columns[t * LANES : (t + 1) * LANES, :]
        columns[t * LANES : (t + 1) * LANES, :] = found

    def columns_of(starts, count, more):
        return [functools.partial(column, t, starts, count, more) for t in range(types)]

    def gather(starts, count, more):
        for work in columns_of(starts, count, more):
            work()

    weave(
        climb(),
        (local_levels + 1) // 2,
        [functools.partial(pick_far, g) for g in range(n // (2 * per_row))],
    )

    @pl.when(late)
    def _():
        first_sends()

    send_root(0, me)

    @pl.when(mine > 0)
    def _():
        send_far(0, team, True)

    @pl.when(lax.rem(me, team) < team - 1)
    def _():
        pl.semaphore_wait(above.at[mine], team - 1 - lax.rem(me, team))
        halo_copy(1).start()

    send_root(me + 1, (mine + 1) * team)
    send_near(mine)

    @pl.when(mine + 1 < teams)
    def _():
        pl.semaphore_wait(above.at[mine + 1], team)

        @pl.when(lax.rem(me, team) == team - 1)
        def _():
            halo_copy(1).start()

        send_near(mine + 1)
        send_root((mine + 1) * team, (mine + 2) * team)

    def send_own():
        send_far(mine * team, (mine + 1) * team, True)
        send_far(n, n + team, False)

    send_far(jnp.minimum(mine, 1) * team, mine * team, True)

    @pl.when(mine == 0)
    def _():
        send_own()


    for copy in loads[8:]:
        copy.wait()

    v = far_ref[...]
    behind = v - cells
    sender = behind // cap
    slot = behind % cap
    delta = sender - me
    hop = jnp.where(delta < 0, delta + PEERS, delta + PEERS - 1)
    position = jnp.where(
        v < cells,
        v,
        jnp.where(
            slot < CAP_FAR,
            close + sender * CAP_FAR + slot,
            cells + hop * rest + slot - CAP_FAR,
        ),
    )
    total = source.shape[1]
    blocks = total // 256
    for b in range(blocks):
        rel[b, :types, :] = jnp.clip(position - 256 * b, -1, 256).astype(F32)

    w = near_ref[...]
    near_rel[0, :kinds, :] = jnp.clip(w - HALO, -1, cells).astype(F32)
    near_rel[1, :kinds, :] = jnp.where(
        w < HALO, w, jnp.where(w >= HALO + cells, w - cells, -1)
    ).astype(F32)
    slips = slip_ref[...]

    def wait_team(index, own):
        start = pl.multiple_of(index * 256, 256)
        if own:
            far_rows(start, 256 - CAP_FAR, index).wait_recv()
        else:
            far_rows(start, 256, index).wait_recv()
        source[:, pl.ds(close + start, 256)] = far_buf[pl.ds(start, 256), :].astype(F32).T.astype(BF)
        return close // 256 + index

    prepare()

    def descend(x):
        high, low = halves(x)
        return mm(high, w_down[:LANES, :]) + mm(high, w_down[LANES:, :]) + mm(low, w_down[:LANES, :])

    def descend2(x):
        high, low = halves(x)
        return mm(high, w_down2[:LANES, :]) + mm(high, w_down2[LANES:, :]) + mm(low, w_down2[:LANES, :])

    def settle():
        spread(bases[1], bases[-1], 0)
        yield
        expansion = None
        for height in reversed(range(local_levels)):
            m = max((cells >> height) // 2, 8)
            both = None if expansion is None else descend(expansion)
            if height >= 1:
                term = terms[local_spots[height] : local_spots[height] + m, :]
                both = term if both is None else both + term
            own_loc[pl.ds(0, m, stride=2), :] = both[:, :LANES]
            own_loc[pl.ds(1, m, stride=2), :] = both[:, LANES:]
            expansion = own_loc[: max(cells >> height, 8), :]
            yield

    def lay(t):
        leaf_cat[:coef, t * LANES : t * LANES + coef] = leaf_ref[t]

    def own_work():
        weave(
            settle(),
            local_levels + 1,
            columns_of([0], cells // 256, False)
            + [functools.partial(beside_own, k) for k in range(kinds)]
            + [functools.partial(lay, t) for t in range(types)],
        )

    @pl.when(mine == 0)
    def _():
        own_work()

    def send_rest(index, carry):
        pl.semaphore_wait(above.at[index], team)
        send_root(index * team, (index + 1) * team)
        return carry

    lax.fori_loop(mine + 2, teams, send_rest, 0)
    send_far((mine + 1) * team, n, False)

    @pl.when(mine > 0)
    def _():
        send_own()


    @pl.when(mine > 0)
    def _():
        own_work()


    def wait_near(side):
        for count in range(1, PEERS + 1):
            @pl.when(near_count(side, count))
            def _():
                near_rows(side, count).wait_recv()

    split = (close - cells) // 2 + cells
    split = -(-split // 256) * 256

    def land_near(start, stop):
        source[:, start:stop] = near_buf[start - cells : stop - cells, :].astype(F32).T.astype(BF)

    wait_near(1)
    land_near(split, close)
    gather([split // 256], (close - split) // 256, True)

    wait_near(0)
    for side in (0, 1):
        @pl.when(inside(-1 if side else 1))
        def _():
            halo_copy(side).wait_recv()

    land_near(cells, split)
    side_slips = jnp.concatenate(
        [halo[...], jnp.zeros((LANES - 2 * HALO, LANES), BF)], axis=0
    ).astype(F32).T.astype(BF)
    stress = jnp.zeros(out_ref.shape, F32)
    for k in range(kinds):
        beside = near_cols[k * LANES : (k + 1) * LANES, :] + mm(
            side_slips, one_hot(LANES, near_rel[1, k : k + 1, :])
        ).astype(BF)
        stress = stress + mm(nb_ref[k], beside)
    out_ref[...] = stress
    gather([cells // 256], (split - cells) // 256, True)

    tops = [0]
    for bit in range(tree_bits):
        tops.append(tops[-1] + max(n >> bit, 32))
    top_spot = local_spots[-1]

    def whole_tree():
        place(0, roots[:, 0, :])
        for _ in rise(tops, [n >> bit for bit in range(tree_bits)], tree_bits - 1):
            yield
        spread(0, tops[-1], top_spot)
        yield

        def chosen(bit):
            both = terms[pl.ds(top_spot + tops[bit] // 2 + (me >> (bit + 1)), 1), :]
            both = jnp.broadcast_to(both, (8, 2 * LANES))
            return jnp.where((me >> bit) & 1 == 0, both[:, :LANES], both[:, LANES:])

        def half(both, bit):
            return jnp.where((me >> bit) & 1 == 0, both[:, :LANES], both[:, LANES:])

        line = lax.broadcasted_iota(jnp.int32, (8, LANES), 0)
        expansion = chosen(tree_bits - 1)
        bit = tree_bits - 2
        if tree_bits % 2 == 0 and bit >= 0:
            expansion = half(descend(expansion), bit) + chosen(bit)
            bit -= 1
            yield
        uppers = range(bit, 0, -2)
        aside = jnp.zeros((8, LANES), F32)
        for i, k in enumerate(uppers):
            aside = jnp.where(line == i, chosen(k), aside)
        aside = descend(aside)
        for i, k in enumerate(uppers):
            quarter = descend2(expansion)
            pair_half = jnp.where((me >> k) & 1 == 0, quarter[:, : 2 * LANES], quarter[:, 2 * LANES :])
            pair_half = pair_half + jnp.broadcast_to(aside[i : i + 1, :], pair_half.shape)
            expansion = half(pair_half, k - 1) + chosen(k - 1)
            yield
        rows = 1
        if local_levels % 2:
            both = descend(expansion)
            for c in range(2):
                loc[pl.ds(c, 8, stride=2), :] = both[:, c * LANES : (c + 1) * LANES]
            rows = 2
            expansion = loc[:8, :]
            yield
        while rows < cells:
            m = max(rows, 8)
            four = descend2(expansion)
            for c in range(4):
                loc[pl.ds(c, m, stride=4), :] = four[:, c * LANES : (c + 1) * LANES]
            rows *= 4
            expansion = loc[: max(rows, 8), :]
            yield

    root_rows().wait_recv()
    weave(
        whole_tree(),
        tree_bits + local_levels // 2,
        columns_of([wait_team(mine, True)], 1, True),
    )

    if teams <= 4:
        gather([wait_team(mine ^ i, False) for i in range(1, teams - 1)], 1, True)
        last = wait_team(mine ^ (teams - 1), False)
    else:
        def middle(i, carry):
            gather([wait_team(mine ^ i, False)], 1, True)
            return carry

        lax.fori_loop(1, teams - 1, middle, 0)
        last = wait_team(mine ^ (teams - 1), False)

    expansion_sum[...] = (loc[...] + own_loc[...]).T
    works = columns_of([last], 1, True)
    parts_of = 2
    marks = [types * i // parts_of for i in range(parts_of + 1)]
    for first, stop in zip(marks[:-1], marks[1:]):
        for work in works[first:stop]:
            work()
        span = slice(first * LANES, stop * LANES)
        found = expansion_sum[...] + mm(leaf_cat[:, span], columns[span, :])
        if stop < types:
            expansion_sum[...] = found
    local_exp = found[:coef].astype(BF)
    out_ref[...] = out_ref[...] + mm(ts_ref[...], local_exp)

    far_rows(0, (n - 1) * CAP_FAR, 0).wait_send()
    root_rows().wait_send()
    for side in (0, 1):
        for count in range(1, PEERS + 1):
            @pl.when(near_count(side, count))
            def _():
                near_rows(side, count).wait_send()

    for side in (0, 1):
        @pl.when(inside(1 if side else -1))
        def _():
            halo_copy(side).wait_send()


def round_up(value, unit):
    return -(-value // unit) * unit


def body(*args):
    args = list(args)
    n = lax.axis_size("leaf")
    cells = args[0].shape[1]
    cap = args[8].shape[1] // n
    for i in (2, 3, 4):
        args[i] = jnp.transpose(args[i], (1, 0, 2))
    args[8] = jnp.reshape(args[8], (n, cap))
    slip, far_list, near_list = args[0], args[9], args[10]
    rest = cap - CAP_FAR
    peers = len(OFFSETS)
    total = cells + n * CAP_FAR + peers * rest
    dma = pltpu.SemaphoreType.DMA
    return pl.pallas_call(
        functools.partial(kernel, n, cells, cap),
        out_shape=pltpu.VMEM(slip.shape, F32),
        in_specs=[pl.BlockSpec(memory_space=pl.ANY)] * len(args),
        out_specs=pl.BlockSpec(memory_space=pltpu.VMEM),
        scratch_shapes=[pltpu.VMEM(a.shape, a.dtype) for a in args] + [
            pltpu.VMEM((n * CAP_FAR, LANES), BF),
            pltpu.VMEM((peers * cap, LANES), BF),
            pltpu.VMEM((n * CAP_FAR, LANES), BF),
            pltpu.VMEM((peers * rest, LANES), BF),
            pltpu.VMEM((2, HALO, LANES), BF),
            pltpu.VMEM((2 * HALO, LANES), BF),
            pltpu.VMEM((1, LANES), F32),
            pltpu.VMEM((n, 1, LANES), F32),
            pltpu.VMEM((n, cap), F32),
            pltpu.VMEM((n * CAP_FAR // LANES, LANES), F32),
            pltpu.VMEM((6, LANES, LANES), F32),
            pltpu.VMEM((2 * LANES, 2 * LANES), BF),
            pltpu.VMEM((2, 2 * LANES, 2 * LANES), BF),
            pltpu.VMEM((2 * LANES, 2 * LANES), BF),
            pltpu.VMEM((4 * LANES, 2 * LANES), BF),
            pltpu.VMEM((2 * LANES, 4 * LANES), BF),
            pltpu.VMEM((2 * cells + 2 * n + 512, LANES), F32),
            pltpu.VMEM((cells + n + 512, 2 * LANES), F32),
            pltpu.VMEM((cells, LANES), F32),
            pltpu.VMEM((cells, LANES), F32),
            pltpu.VMEM((LANES, cells), F32),
            pltpu.VMEM((total // 256, round_up(far_list.shape[0], 8), cells), F32),
            pltpu.VMEM((2, round_up(near_list.shape[0], 8), cells), F32),
            pltpu.VMEM((LANES, total), BF),
            pltpu.VMEM((LANES, far_list.shape[0] * LANES), BF),
            pltpu.VMEM((far_list.shape[0] * LANES, cells), BF),
            pltpu.VMEM((near_list.shape[0] * LANES, cells), BF),
            dma((len(args),)),
            pltpu.SemaphoreType.REGULAR((n * CAP_FAR // 256,)),
            dma,
            dma((n * CAP_FAR // 256,)),
            dma((2,)),
            dma((2,)),
            dma((2,)),
            dma((2,)),
            dma,
            dma,
        ],
        compiler_params=pltpu.CompilerParams(collective_id=0, has_side_effects=True),
    )(*args)


def solution(mesh):
    return jax.shard_map(
        body,
        mesh=mesh,
        in_specs=(
            P(None, "leaf"),
            P(),
            P(),
            P(),
            P(),
            P(),
            P(),
            P(),
            P("leaf", None),
            P(None, "leaf"),
            P(None, "leaf"),
        ),
        out_specs=P(None, "leaf"),
        check_vma=False,
    )
```
